256 devices in a mesh: dp: 8 (over x, core), expert: 32 (over y, z).
Axes of the slice: x: 4, y: 4, z: 8, core: 2. Of those that a mesh axis runs over, the one named last changes fastest.
Arguments:
- queries: bfloat16 [2048, 16, 3072], P('expert', 'dp'), may hold values from -256 to 256
- key_nope: bfloat16 [2048, 16, 2048], P('expert', 'dp'), may hold values from -4 to 4
- key_rope: bfloat16 [2048, 16, 64], P('expert', 'dp'), may hold values from -4 to 4
- values: bfloat16 [2048, 16, 2048], P('expert', 'dp'), may hold values from -6 to 6
- residual: bfloat16 [2048, 16, 2048], P('expert', 'dp'), may hold values from -6 to 6
- segments: int32 [16, 2048], P('dp'), may hold values from 0 to 1, never falling along the last dimension, each value on 1 to 1536 neighbouring positions
- out_proj: bfloat16 [2048, 2048], P(('dp', 'expert')), may hold values from -0.125 to 0.125
- norm_gain: bfloat16 [2048], replicated, may hold values from 0.5 to 1.5
- expert_gate: bfloat16 [32, 2048, 704], P('expert'), may hold values from -0.125 to 0.125
- expert_up: bfloat16 [32, 2048, 704], P('expert'), may hold values from -0.125 to 0.125
- expert_down: bfloat16 [32, 704, 2048], P('expert'), may hold values from -0.21875 to 0.21875
- routes: int32 [8, 32, 128, 6], P('dp', 'expert'), may hold values from 0 to 31, all different within a row; in each aligned block of 128 rows (0 to 127, 128 to 255, ..., all dimensions but the last counted through in order) at most 36 rows name the same one
- route_weights: float32 [8, 32, 128, 6], P('dp', 'expert'), may hold values from 0.1 to 0.6
Outputs:
- layer_out: bfloat16 [2048, 16, 2048], P('expert', 'dp')
The draws below stay inside these ranges and needn't reach their ends.
Inputs may be any that keep to these rules, and one draw needn't show every extreme that they name: `routes`: each row names 6 different experts; within the rows of one device no expert is named more than 36 times.
All inputs are finite; a program needn't handle non-finite values.
Results may differ from the reference program's by a relative error of at most 0.0049.
Values may be sent and summed in bfloat16 or wider, within the bound.
No kernel may reach another device: no remote copies, remote signals or barrier semaphores. Data moves between devices by JAX's collectives and lax.ppermute only.
A program may use at most 128 MiB of HBM per device.

```python
import math
import jax
import jax.numpy as jnp
import numpy as np
from jax import lax

D = 2048
HEADS = 16
NOPE = 128
ROPE = 64
V_DIM = 128
FF_E = 704
TOP = 6
STREAMS = 2
DOCS = 2
TOK_HALF = 64
QK_DIM = 192
EXPERTS = 32
LENGTH = 2048
S_ALL = 16
TOK_DEV = 128
MOST = 36
DOC_MOST = 1536
N_DP = 8
N_EXPERT = 32


def key_parts(key):
    nope_part = jnp.clip(jax.random.normal(jax.random.fold_in(key, 11), (LENGTH, S_ALL, HEADS * NOPE), jnp.float32), -4.0, 4.0)
    rope_part = jnp.clip(jax.random.normal(jax.random.fold_in(key, 12), (LENGTH, S_ALL, ROPE), jnp.float32), -4.0, 4.0)
    return (nope_part, rope_part)


def draw_key_nope(key, part):
    return key_parts(key)[0].astype(jnp.bfloat16)


def draw_key_rope(key, part):
    return key_parts(key)[1].astype(jnp.bfloat16)


def draw_queries(key, part):
    drawn = jnp.clip(jax.random.normal(jax.random.fold_in(key, 15), (LENGTH, S_ALL, HEADS * QK_DIM), jnp.float32), -6.0, 6.0)
    return drawn.astype(jnp.bfloat16)


def steps_of(key, dims, shards, smallest, largest):
    def one(axis_at, shards_of):
        heights = jax.random.uniform(jax.random.fold_in(jax.random.fold_in(key, 6), axis_at), (shards_of,), jnp.float32, smallest / len(shards), largest / len(shards))
        return jnp.repeat(jnp.exp(heights), dims[axis_at] // shards_of).reshape((-1,) + (1,) * (len(dims) - axis_at - 1))

    loudness = one(*shards[0])
    for cut in shards[1:]:
        loudness = loudness * one(*cut)
    return loudness


def profile(amount, total, bound, skew):
    portions = [(1 << 20) // math.isqrt(rank ** skew) + 1 for rank in range(2, amount + 1)]
    surplus, given = total - bound - (amount - 1), [1] * (amount - 1)
    while surplus > 0:
        movable = [i for i in range(amount - 1) if given[i] < bound]
        mass, budget = sum([portions[i] for i in movable]), surplus
        for i in movable:
            more = min(bound - given[i], max(1, budget * portions[i] // mass), surplus)
            given[i] = given[i] + more
            surplus = surplus - more
    return np.array([bound] + given)


def uneven(own_key, count, total, most, lean):
    if count == 2:
        one = jax.random.randint(own_key, (), max(1, total - most), min(most, total - 1) + 1)
        return jnp.stack([one, total - one])
    sizes = jnp.asarray(profile(count, total, most, lean), jnp.int32)
    twos = (count - 1) // 2
    giver, receiver = sizes[1:1 + 2 * twos:2], sizes[2:2 + 2 * twos:2]
    slack = jnp.minimum(giver - 1, most - receiver)
    passed = jax.random.randint(jax.random.fold_in(own_key, 1), (twos,), 0, 1 << 20) % (slack + 1)
    sizes = sizes.at[1:1 + 2 * twos:2].set(giver - passed).at[2:2 + 2 * twos:2].set(receiver + passed)
    return sizes[jax.random.permutation(jax.random.fold_in(own_key, 2), count)]


def routed_block(key, own, number, rows, count, top, most, slope):
    ranking = jax.random.permutation(key, count)
    heavy_load, usual = portions_of(count, rows * top, most, slope, True), portions_of(count, rows * top, most, slope, False)
    places = jnp.arange(count)

    def named(lengths, rotation):
        used = int((lengths > 0).sum())
        fixed = max(1, used // 4)
        passed = fixed + (places - fixed + rotation * (used - fixed)) % max(1, count - fixed)
        return jnp.zeros((count,), jnp.int32).at[ranking[jnp.where(places < fixed, places, passed)]].set(jnp.asarray(lengths, jnp.int32))

    lengths = jnp.where(number % 4 == 0, named(heavy_load, number // 4), named(usual, number - number // 4 - 1))
    mixed = jax.random.permutation(jax.random.fold_in(own, 3), count)
    source_of, receiver = mixed[0:count // 2 * 2:2], mixed[1:count // 2 * 2:2]
    margin = jnp.minimum(lengths[source_of] - 1, most - lengths[receiver]) // 2
    margin = jnp.where((source_of == ranking[0]) | (receiver == ranking[0]) | (lengths[receiver] == 0), 0, jnp.maximum(margin, 0))
    passed = jax.random.randint(jax.random.fold_in(own, 4), (count // 2,), 0, 1 << 20) % (margin + 1)
    lengths = lengths.at[source_of].add(-passed).at[receiver].add(passed)
    labels = jnp.searchsorted(jnp.cumsum(lengths), jnp.arange(rows * top), side="right").astype(jnp.int32)
    grid = labels.reshape(top, rows).T
    grid = grid[jax.random.permutation(jax.random.fold_in(own, 1), rows)]
    rotation = jax.random.randint(jax.random.fold_in(own, 2), (rows, 1), 0, top)
    return jnp.take_along_axis(grid, (jnp.arange(top)[None, :] + rotation) % top, axis=1)


def portions_of(number_of, total, most, lean, full):
    loads = [(1 << 20) // math.isqrt(standing ** lean) + 1 for standing in range(1, number_of + 1)]
    largest = most if full else min(most, max(-(-total // number_of), total * loads[0] // sum(loads)))
    least = 1 if total - largest >= number_of - 1 else 0
    counts, surplus = [largest] + [least] * (number_of - 1), total - largest - least * (number_of - 1)
    while surplus > 0:
        free = [i for i in range(1, number_of) if counts[i] < largest] or [i for i in range(1, number_of) if counts[i] < most]
        pool, left = sum([loads[i] for i in free]), surplus
        for i in free:
            extra = min(most - counts[i], max(1, left * loads[i] // pool), surplus)
            counts[i] = counts[i] + extra
            surplus = surplus - extra
    return np.array(counts)


def normal_values(own_key, extent, scale, most, shards=(), held_as=jnp.bfloat16):
    values = scale * jax.random.normal(own_key, extent, jnp.float32)
    if shards:
        values = values * steps_of(own_key, extent, shards, -0.22, 0.18)
    return jnp.clip(values, -most, most).astype(held_as)


def setup_inputs(seed: int = 0) -> dict:
    streams_of = jax.random.split(jax.random.key(seed), 14)
    queries = draw_queries(jax.random.fold_in(streams_of[13], 71), 0)
    key_nope = draw_key_nope(jax.random.fold_in(streams_of[13], 71), 0)
    key_rope = draw_key_rope(jax.random.fold_in(streams_of[13], 71), 0)
    values = normal_values(streams_of[3], (LENGTH, S_ALL, HEADS * V_DIM), 1.0, 6.0, ((0, 32), (1, 8)))
    residual = normal_values(streams_of[4], (LENGTH, S_ALL, D), 1.0, 6.0, ((0, 32), (1, 8)))
    segments = jax.vmap(lambda own: jnp.searchsorted(jnp.cumsum(uneven(own, DOCS, LENGTH, DOC_MOST, 1)), jnp.arange(LENGTH), side="right"))(jax.random.split(streams_of[5], S_ALL)).reshape((S_ALL, LENGTH)).astype(jnp.int32)
    out_proj = normal_values(streams_of[6], (HEADS * V_DIM, D), (HEADS * V_DIM) ** -0.5, 0.125, ((0, 256),))
    norm_gain = jnp.clip(1.0 + 0.1 * jax.random.normal(streams_of[7], (D,), jnp.float32), 0.5, 1.5).astype(jnp.bfloat16)
    expert_gate = normal_values(streams_of[8], (EXPERTS, D, FF_E), D ** -0.5, 0.125, ((0, 32),))
    expert_up = normal_values(streams_of[9], (EXPERTS, D, FF_E), D ** -0.5, 0.125, ((0, 32),))
    expert_down = normal_values(streams_of[10], (EXPERTS, FF_E, D), FF_E ** -0.5, 0.21875, ((0, 32),))
    routes_keys = jax.random.split(jax.random.fold_in(streams_of[11], 1), N_DP * N_EXPERT * TOK_DEV // TOK_DEV)
    routes_turns = jax.random.permutation(jax.random.fold_in(streams_of[11], 3), N_DP * N_EXPERT * TOK_DEV // TOK_DEV)
    routes = jax.vmap(lambda own, number: routed_block(jax.random.fold_in(streams_of[11], 2), own, number, TOK_DEV, EXPERTS, TOP, MOST, 1))(routes_keys, routes_turns).reshape((N_DP, N_EXPERT, TOK_DEV, TOP))
    route_weights = jnp.clip(0.1 + 0.5 * jax.random.uniform(streams_of[12], (N_DP, N_EXPERT, TOK_DEV, TOP), jnp.float32) ** steps_of(streams_of[12], (N_DP, N_EXPERT, TOK_DEV, TOP), ((0, 8), (1, 32)), -0.2, 0.2), 0.1, 0.6)
    return dict(queries=queries, key_nope=key_nope, key_rope=key_rope, values=values, residual=residual, segments=segments, out_proj=out_proj, norm_gain=norm_gain, expert_gate=expert_gate, expert_up=expert_up, expert_down=expert_down, routes=routes, route_weights=route_weights)


EPSILON = 1e-06

def to_streams(block_array):
    width = block_array.shape[-1]
    shaped = block_array.reshape(N_DP, N_EXPERT, TOK_HALF, STREAMS, width)
    shaped = jnp.transpose(shaped, (1, 2, 0, 3, 4))
    return shaped.reshape(LENGTH, S_ALL, width)

def feed_forward(rows, gate_matrix, up_matrix, down_matrix):
    gate_part = jnp.dot(rows, gate_matrix, preferred_element_type=jnp.float32)
    up_part = jnp.dot(rows, up_matrix, preferred_element_type=jnp.float32)
    activated = (jax.nn.silu(gate_part) * up_part).astype(jnp.bfloat16)
    return jnp.dot(activated, down_matrix, preferred_element_type=jnp.float32).astype(jnp.bfloat16)

def attend_stream(inputs):
    query_rows, nope_rows, rope_rows, value_rows, segment_row = inputs
    query_heads = query_rows.reshape(LENGTH, HEADS, QK_DIM).astype(jnp.float32)
    key_heads = jnp.concatenate([nope_rows.reshape(LENGTH, HEADS, NOPE), jnp.broadcast_to(rope_rows[:, None, :], (LENGTH, HEADS, ROPE))], axis=2).astype(jnp.float32)
    value_heads = value_rows.reshape(LENGTH, HEADS, V_DIM).astype(jnp.float32)
    scores = jnp.einsum('qhd,khd->hqk', query_heads, key_heads) * QK_DIM ** (-0.5)
    positions = jnp.arange(LENGTH, dtype=jnp.int32)
    allowed = (positions[:, None] >= positions[None, :]) & (segment_row[:, None] == segment_row[None, :])
    scores = jnp.where(allowed[None], scores, -jnp.inf)
    row_peak = lax.optimization_barrier(jnp.max(scores, axis=2, keepdims=True))
    raised = jnp.exp(scores - row_peak)
    probs = (raised / lax.optimization_barrier(jnp.sum(raised, axis=2, keepdims=True))).astype(jnp.bfloat16)
    mixed = jnp.einsum('hqk,khd->qhd', probs.astype(jnp.float32), value_heads)
    return mixed.reshape(LENGTH, HEADS * V_DIM).astype(jnp.bfloat16)

def reference(queries, key_nope, key_rope, values, residual, segments, out_proj, norm_gain, expert_gate, expert_up, expert_down, routes, route_weights):
    inputs = (jnp.swapaxes(queries, 0, 1), jnp.swapaxes(key_nope, 0, 1), jnp.swapaxes(key_rope, 0, 1), jnp.swapaxes(values, 0, 1), segments)
    attended = lax.map(attend_stream, inputs)
    token_count = LENGTH * S_ALL
    attn_rows = jnp.swapaxes(attended, 0, 1).reshape(token_count, HEADS * V_DIM)
    projected = jnp.dot(attn_rows, out_proj, preferred_element_type=jnp.float32)
    hidden = residual.reshape(token_count, D).astype(jnp.float32) + projected
    mean_square = lax.optimization_barrier(jnp.mean(hidden * hidden, axis=1, keepdims=True))
    normed = (hidden * lax.rsqrt(mean_square + EPSILON) * norm_gain.astype(jnp.float32)).astype(jnp.bfloat16)
    chosen = to_streams(routes).reshape(token_count, TOP)
    scales = to_streams(route_weights).reshape(token_count, TOP)
    capacity = min(N_DP * N_EXPERT * MOST, token_count)
    row_ids = jnp.arange(token_count, dtype=jnp.int32)

    def one_expert(routed_total, expert_inputs):
        gate_matrix, up_matrix, down_matrix, expert_id = expert_inputs
        matches = chosen == expert_id
        picked = jnp.any(matches, axis=1)
        weight_row = lax.optimization_barrier(jnp.sum(jnp.where(matches, scales, jnp.zeros_like(scales)), axis=1))
        live_order = (jnp.cumsum(picked.astype(jnp.int32)) - 1).astype(jnp.int32)
        live_place = jnp.where(picked, live_order, capacity).astype(jnp.int32)
        source_rows = jnp.zeros((capacity,), jnp.int32).at[live_place].set(row_ids, mode='drop')
        filled = jnp.zeros((capacity,), jnp.int32).at[live_place].set(1, mode='drop')
        outputs = feed_forward(normed[source_rows], gate_matrix, up_matrix, down_matrix)
        contribution = (filled > 0)[:, None] * weight_row[source_rows][:, None] * outputs.astype(jnp.float32)
        return (routed_total.at[source_rows].add(contribution), expert_id)
    expert_ids = jnp.arange(EXPERTS, dtype=jnp.int32)
    routed_total = lax.scan(one_expert, jnp.zeros((token_count, D), jnp.float32), (expert_gate, expert_up, expert_down, expert_ids))[0]
    layer_out = (hidden + routed_total).astype(jnp.bfloat16)
    return layer_out.reshape(LENGTH, S_ALL, D)
```

```python
import jax
import jax.numpy as jnp
from jax import lax
from jax.experimental import pallas as pl
from jax.experimental.pallas import tpu as pltpu
from jax.sharding import PartitionSpec as P


HEADS = 16
NOPE = 128
ROPE = 64
V_DIM = 128
TOP = 6
EPSILON = 1e-06


N_DP = 8
N_X = 4
N_Y = 4
N_Z = 8
N_EXPERT = N_Y * N_Z
STREAMS = 2
T_DEV = 64
TOK = STREAMS * T_DEV
SLOTS = 36
PAIR = 2 * SLOTS
D = 2048
FF = 704
LENGTH = 2048
META = 8
BLOCK = TOK + META
VMEM = pltpu.MemorySpace.VMEM
BF = jnp.bfloat16
F32 = jnp.float32


def params(mib=40):
    return pltpu.CompilerParams(vmem_limit_bytes=mib << 20)


def whole(n):
    return [pl.BlockSpec(memory_space=VMEM) for _ in range(n)]


def pack_kernel(q_ref, k_ref, r_ref, v_ref, out_ref):
    for s in range(STREAMS):
        rope = r_ref[:, s, :]
        for h in range(HEADS):
            i = s * HEADS + h
            at = h * (NOPE + ROPE)
            out_ref[i, 0:64, :] = q_ref[:, s, at : at + NOPE]
            out_ref[i, 64:128, :] = k_ref[:, s, h * NOPE : (h + 1) * NOPE]
            out_ref[i, 128:192, :] = v_ref[:, s, h * V_DIM : (h + 1) * V_DIM]
            out_ref[i, 192:256, :] = jnp.concatenate(
                [q_ref[:, s, at + NOPE : at + NOPE + ROPE], rope], axis=1
            )


def pack(q, k, r, v):
    return pl.pallas_call(
        pack_kernel,
        out_shape=jax.ShapeDtypeStruct((32, 256, 128), BF),
        in_specs=whole(4),
        out_specs=pl.BlockSpec(memory_space=VMEM),
        compiler_params=params(),
        name="pack",
    )(q, k, r, v)


QB = 256


def attend_kernel(split_ref, x_ref, o_ref, k_scr, v_scr):
    scale = (NOPE + ROPE) ** -0.5
    split = split_ref[0]
    log2e = 1.4426950408889634
    zero = jnp.zeros((T_DEV, ROPE), BF)
    for e in range(N_EXPERT):
        rows = slice(e * T_DEV, (e + 1) * T_DEV)
        k_scr[rows, 0:NOPE] = x_ref[e, 64:128, :]
        k_scr[rows, NOPE:256] = jnp.concatenate([x_ref[e, 192:256, 64:128], zero], axis=1)
        v_scr[rows, :] = x_ref[e, 128:192, :]
    per = QB // T_DEV
    for b in range(LENGTH // QB):
        n = (b + 1) * QB
        q = jnp.concatenate(
            [
                jnp.concatenate([x_ref[b * per + j, 0:64, :] for j in range(per)], axis=0),
                jnp.concatenate([x_ref[b * per + j, 192:256, :] for j in range(per)], axis=0),
            ],
            axis=1,
        )
        lane = lax.broadcasted_iota(jnp.int32, (QB, 256), 1)
        q = jnp.where(lane < NOPE + ROPE, q, jnp.zeros_like(q))
        scores = lax.dot_general(
            q, k_scr[0:n, :], (((1,), (1,)), ((), ())), preferred_element_type=F32
        )
        row = b * QB + lax.broadcasted_iota(jnp.int32, (QB, 1), 0)
        col = lax.broadcasted_iota(jnp.int32, (QB, n), 1)
        low = jnp.where(row >= split, split, 0)
        scores = jnp.where((col <= row) & (col >= low), scores, -1e30)
        peak = jnp.max(scores, axis=1, keepdims=True)
        raised = jnp.exp2((scores - peak) * (scale * log2e))
        total = jnp.sum(raised, axis=1, keepdims=True)
        mixed = jnp.dot(raised.astype(BF), v_scr[0:n, :], preferred_element_type=F32)
        mixed = (mixed / total).astype(BF)
        for j in range(per):
            o_ref[b * per + j] = mixed[j * T_DEV : (j + 1) * T_DEV, :]


def attend(split, x):
    return pl.pallas_call(
        attend_kernel,
        out_shape=jax.ShapeDtypeStruct((32, T_DEV, V_DIM), BF),
        in_specs=[pl.BlockSpec(memory_space=pltpu.MemorySpace.SMEM)] + whole(1),
        out_specs=pl.BlockSpec(memory_space=VMEM),
        scratch_shapes=[pltpu.VMEM((LENGTH, 256), BF), pltpu.VMEM((LENGTH, V_DIM), BF)],
        compiler_params=params(),
        name="attend",
    )(split, x)


PIECE = D // N_DP


def place_kernel(at_ref, *refs):
    pieces, out_ref = refs[:-1], refs[-1]
    n, rows = len(pieces), pieces[0].shape[0]
    for k, piece in enumerate(pieces):
        start = pl.multiple_of(lax.rem(at_ref[0] + (n - k), n) * rows, rows)
        out_ref[pl.ds(start, rows), :] = piece[...]


def place(at, pieces):
    rows = pieces[0].shape[0] * len(pieces)
    return pl.pallas_call(
        place_kernel,
        out_shape=jax.ShapeDtypeStruct((rows, D), BF),
        in_specs=[pl.BlockSpec(memory_space=pltpu.MemorySpace.SMEM)] + whole(len(pieces)),
        out_specs=pl.BlockSpec(memory_space=VMEM),
        compiler_params=params(16),
        name="place",
    )(at, *pieces)


def project_kernel(which_ref, x_ref, *refs):
    w_refs = refs[:N_DP]
    res_ref, gain_ref, meta_ref, hid_ref, norm_ref = refs[N_DP:]
    acc = jnp.concatenate([res_ref[:, s, :] for s in range(STREAMS)], axis=0).astype(F32)
    for k in range(N_DP):
        first = which_ref[k] * (PIECE // V_DIM)
        a = jnp.concatenate(
            [
                jnp.concatenate([x_ref[s, first + j] for j in range(PIECE // V_DIM)], axis=1)
                for s in range(STREAMS)
            ],
            axis=0,
        )
        acc = acc + jnp.dot(a, w_refs[k][...], preferred_element_type=F32)
    hid_ref[...] = acc
    mean = jnp.mean(acc * acc, axis=1, keepdims=True)
    normed = acc * lax.rsqrt(mean + EPSILON) * gain_ref[...].astype(F32)
    norm_ref[0:TOK, :] = normed.astype(BF)
    norm_ref[TOK:BLOCK, :] = meta_ref[...]


def project(which, x, ws, res, gain, meta):
    return pl.pallas_call(
        project_kernel,
        out_shape=(
            jax.ShapeDtypeStruct((TOK, D), F32),
            jax.ShapeDtypeStruct((BLOCK, D), BF),
        ),
        in_specs=[pl.BlockSpec(memory_space=pltpu.MemorySpace.SMEM)] + whole(4 + N_DP),
        out_specs=whole(2),
        compiler_params=params(),
        name="project",
    )(which, x.reshape(STREAMS, HEADS, T_DEV, V_DIM), *ws, res, gain, meta)


def one_hot(meta, expert):
    named = meta[:, 0:TOK].astype(F32)
    rows = lax.broadcasted_iota(jnp.int32, named.shape, 0)
    match = jnp.where((named == expert) & (rows < TOP), 1.0, 0.0)
    member = jnp.sum(match, axis=0, keepdims=True)
    token = lax.broadcasted_iota(jnp.int32, (TOK, TOK), 0)
    other = lax.broadcasted_iota(jnp.int32, (TOK, TOK), 1)
    before = jnp.where(token < other, 1.0, 0.0).astype(BF)
    rank = jnp.dot(
        jnp.broadcast_to(member, (8, TOK)).astype(BF), before, preferred_element_type=F32
    )[0:1, :]
    slot = lax.broadcasted_iota(jnp.int32, (SLOTS, TOK), 0).astype(F32)
    return jnp.where((slot == rank) & (member > 0.5), 1.0, 0.0), match


def select_kernel(at_ref, a_ref, b_ref, *outs):
    y, z = at_ref[0], at_ref[1]
    rows = jnp.concatenate([a_ref[0:TOK, :], b_ref[0:TOK, :]], axis=0)
    none = jnp.zeros((SLOTS, TOK), F32)
    picks = []
    for k in range(N_Y):
        expert = (lax.rem(y + k, N_Y) * N_Z + z).astype(F32)
        hot_a, _ = one_hot(a_ref[TOK:BLOCK, :], expert)
        hot_b, _ = one_hot(b_ref[TOK:BLOCK, :], expert)
        picks.append(
            jnp.concatenate(
                [jnp.concatenate([hot_a, none], axis=1), jnp.concatenate([none, hot_b], axis=1)],
                axis=0,
            ).astype(BF)
        )
    chosen = jnp.dot(jnp.concatenate(picks, axis=0), rows, preferred_element_type=F32).astype(BF)
    for k in range(N_Y):
        outs[k][...] = chosen[k * PAIR : (k + 1) * PAIR, :]


def select(at, a, b):
    return pl.pallas_call(
        select_kernel,
        out_shape=[jax.ShapeDtypeStruct((PAIR, D), BF)] * N_Y,
        in_specs=[pl.BlockSpec(memory_space=pltpu.MemorySpace.SMEM)] + whole(2),
        out_specs=whole(N_Y),
        compiler_params=params(),
        name="select",
    )(at, a, b)


EK = 512


def expert_kernel(x0, x1, x2, x3, gate_ref, up_ref, down_ref, y0, y1, y2, y3, g_scr, u_scr):
    step = pl.program_id(0)
    rows = jnp.concatenate([x[...] for x in (x0, x1, x2, x3)], axis=0)
    across = (((1,), (1,)), ((), ()))
    g = lax.dot_general(rows, gate_ref[0], across, preferred_element_type=F32)
    u = lax.dot_general(rows, up_ref[0], across, preferred_element_type=F32)

    @pl.when(step == 0)
    def _():
        g_scr[...] = g
        u_scr[...] = u

    @pl.when(step > 0)
    def _():
        g_scr[...] += g
        u_scr[...] += u

    @pl.when(step == pl.num_programs(0) - 1)
    def _():
        gate = g_scr[...]
        act = (gate / (1.0 + jnp.exp(-gate)) * u_scr[...]).astype(BF)
        out = jnp.dot(act, down_ref[0], preferred_element_type=F32).astype(BF)
        for k, y in enumerate((y0, y1, y2, y3)):
            y[...] = out[k * PAIR : (k + 1) * PAIR, :]


def expert(xs, gate, up, down):
    return pl.pallas_call(
        expert_kernel,
        grid=(D // EK,),
        out_shape=[jax.ShapeDtypeStruct((PAIR, D), BF)] * N_Y,
        in_specs=[pl.BlockSpec((PAIR, EK), lambda i: (0, i))] * N_Y
        + [
            pl.BlockSpec((1, FF, EK), lambda i: (0, 0, i)),
            pl.BlockSpec((1, FF, EK), lambda i: (0, 0, i)),
            pl.BlockSpec((1, FF, D), lambda i: (0, 0, 0)),
        ],
        out_specs=[pl.BlockSpec((PAIR, D), lambda i: (0, 0))] * N_Y,
        scratch_shapes=[pltpu.VMEM((N_Y * PAIR, FF), F32), pltpu.VMEM((N_Y * PAIR, FF), F32)],
        compiler_params=params(),
        name="expert",
    )(*xs, gate, up, down)


def partials(at_ref, a_ref, b_ref, rets):
    y, z = at_ref[0], at_ref[1]
    rows = jnp.concatenate([r[...] for r in rets], axis=0)
    results = []
    for which, meta_ref in enumerate((a_ref, b_ref)):
        meta = meta_ref[...]
        high = meta[:, TOK : 2 * TOK].astype(F32)
        low = meta[:, 2 * TOK : 3 * TOK].astype(F32)
        highs, lows = [], []
        none = jnp.zeros((SLOTS, TOK), F32)
        for k in range(N_Y):
            e = (lax.rem(y + k, N_Y) * N_Z + z).astype(F32)
            hot, match = one_hot(meta, e)
            hot_high = hot * jnp.sum(match * high, axis=0, keepdims=True)
            hot_low = hot * jnp.sum(match * low, axis=0, keepdims=True)
            highs += [hot_high, none] if which == 0 else [none, hot_high]
            lows += [hot_low, none] if which == 0 else [none, hot_low]
        contract = (((0,), (0,)), ((), ()))
        results.append(
            lax.dot_general(
                jnp.concatenate(highs, axis=0).astype(BF), rows, contract, preferred_element_type=F32
            )
            + lax.dot_general(
                jnp.concatenate(lows, axis=0).astype(BF), rows, contract, preferred_element_type=F32
            )
        )
    return results


def first_kernel(at_ref, a_ref, b_ref, r0, r1, r2, r3, out_a, out_b):
    sum_a, sum_b = partials(at_ref, a_ref, b_ref, (r0, r1, r2, r3))
    out_a[...] = sum_a.astype(BF)
    out_b[...] = sum_b.astype(BF)


def add_kernel(at_ref, a_ref, b_ref, r0, r1, r2, r3, in_a, in_b, out_a, out_b):
    sum_a, sum_b = partials(at_ref, a_ref, b_ref, (r0, r1, r2, r3))
    out_a[...] = (sum_a + in_a[...].astype(F32)).astype(BF)
    out_b[...] = (sum_b + in_b[...].astype(F32)).astype(BF)


def combine(at, a, b, rets, incoming=()):
    metas = [pl.BlockSpec((META, D), lambda i: (TOK // META, 0))] * 2
    rest = [pl.BlockSpec((PAIR, D), lambda i: (0, 0))] * N_Y
    extra = [pl.BlockSpec((TOK, D), lambda i: (0, 0))] * len(incoming)
    return pl.pallas_call(
        add_kernel if incoming else first_kernel,
        grid=(1,),
        out_shape=[jax.ShapeDtypeStruct((TOK, D), BF)] * 2,
        in_specs=[pl.BlockSpec(memory_space=pltpu.MemorySpace.SMEM)] + metas + rest + extra,
        out_specs=[pl.BlockSpec((TOK, D), lambda i: (0, 0))] * 2,
        compiler_params=params(),
        name="combine",
    )(at, a, b, *rets, *incoming)


def last_kernel(at_ref, a_ref, b_ref, r0, r1, r2, r3, in_a, in_b, hid_ref, out_a, out_b):
    sum_a, sum_b = partials(at_ref, a_ref, b_ref, (r0, r1, r2, r3))
    out_a[...] = hid_ref[...] + sum_a + in_a[...].astype(F32)
    out_b[...] = (sum_b + in_b[...].astype(F32)).astype(BF)


def combine_last(at, a, b, rets, in_a, in_b, hidden):
    metas = [pl.BlockSpec((META, D), lambda i: (TOK // META, 0))] * 2
    rest = [pl.BlockSpec((PAIR, D), lambda i: (0, 0))] * N_Y
    extra = [pl.BlockSpec((TOK, D), lambda i: (0, 0))] * 3
    return pl.pallas_call(
        last_kernel,
        grid=(1,),
        out_shape=[
            jax.ShapeDtypeStruct((TOK, D), F32),
            jax.ShapeDtypeStruct((TOK, D), BF),
        ],
        in_specs=[pl.BlockSpec(memory_space=pltpu.MemorySpace.SMEM)] + metas + rest + extra,
        out_specs=[pl.BlockSpec((TOK, D), lambda i: (0, 0))] * 2,
        compiler_params=params(),
        name="combine_last",
    )(at, a, b, *rets, in_a, in_b, hidden)


def along_z(x, k):
    pairs = [(y * N_Z + z, y * N_Z + (z + k) % N_Z) for y in range(N_Y) for z in range(N_Z)]
    return lax.ppermute(x, "expert", pairs)


def along_y(x, k):
    pairs = [(y * N_Z + z, (y + k) % N_Y * N_Z + z) for y in range(N_Y) for z in range(N_Z)]
    return lax.ppermute(x, "expert", pairs)


def along_dp(x, hops, swap):
    pairs = [
        (p * 2 + c, (p + hops) % N_X * 2 + (c + swap) % 2) for p in range(N_X) for c in range(2)
    ]
    return lax.ppermute(x, "dp", pairs)


def meta_rows(routes, route_weights):
    ids = routes.reshape(T_DEV, STREAMS, TOP).transpose(2, 1, 0).reshape(TOP, TOK)
    scales = route_weights.reshape(T_DEV, STREAMS, TOP).transpose(2, 1, 0).reshape(TOP, TOK)
    high = lax.reduce_precision(scales, 8, 7)
    both = jnp.concatenate([ids.astype(F32), high, scales - high], axis=1)
    return jnp.pad(both, ((0, META - TOP), (0, D - 3 * TOK))).astype(BF)


def body(
    queries,
    key_nope,
    key_rope,
    values,
    residual,
    segments,
    out_proj,
    norm_gain,
    expert_gate,
    expert_up,
    expert_down,
    routes,
    route_weights,
):
    me = lax.axis_index("expert")
    at = jnp.stack([me // N_Z, me % N_Z]).astype(jnp.int32)
    meta = meta_rows(routes, route_weights)

    slabs = [out_proj] + [along_z(out_proj, k) for k in range(1, N_Z)]
    sent = pack(queries, key_nope, key_rope, values)
    slabs = place(at[1:2], slabs)
    slabs = [slabs] + [along_y(slabs, k) for k in range(1, N_Y)]
    got = lax.all_to_all(sent, "expert", 0, 0, tiled=True)
    slabs = place(at[0:1], slabs)
    pieces = [slabs] + [along_dp(slabs, k, 0) for k in range(1, N_X)]
    pieces += [along_dp(w, 0, 1) for w in pieces]
    dp = lax.axis_index("dp")
    x, core = dp // 2, dp % 2
    which = jnp.stack(
        [(x + N_X - k) % N_X * 2 + (core + c) % 2 for c in range(2) for k in range(N_X)]
    ).astype(jnp.int32)

    stream = me // HEADS
    ones = jnp.sum(segments, axis=1)
    split = LENGTH - jnp.where(stream == 0, ones[0], ones[1])
    mixed = attend(split.reshape(1), got)
    back = lax.all_to_all(mixed, "expert", 0, 0, tiled=True)
    hidden, own = project(which, back, pieces, residual, norm_gain.reshape(1, D), meta)

    gate_t, up_t = jnp.swapaxes(expert_gate, 1, 2), jnp.swapaxes(expert_up, 1, 2)

    right, left = [own], [own]
    for k in range(1, 5):
        right.append(along_z(right[-1], 1))
        if k < 4:
            left.append(along_z(left[-1], -1))
    blocks = [(own, right[1]), (left[1], right[2]), (left[2], right[3]), (left[3], right[4])]

    rets = []
    for a, b in blocks:
        rows = select(at, a, b)
        xs = [rows[0]] + [along_y(rows[k], k) for k in range(1, N_Y)]
        ys = expert(xs, gate_t, up_t, expert_down)
        rets.append([ys[0]] + [along_y(ys[k], -k) for k in range(1, N_Y)])

    far_a, far_b = combine(at, *blocks[3], rets[3])
    for k in (2, 1):
        arrived = (along_z(far_a, 1), along_z(far_b, -1))
        far_a, far_b = combine(at, *blocks[k], rets[k], arrived)
    arrived = (along_z(far_a, 1), along_z(far_b, -1))
    total, far_b = combine_last(at, *blocks[0], rets[0], *arrived, hidden)
    return finish(total, along_z(far_b, -1))


def finish_kernel(sum_ref, in_ref, out_ref):
    total = sum_ref[...] + in_ref[...].astype(F32)
    for s in range(STREAMS):
        out_ref[:, s, :] = total[s * T_DEV : (s + 1) * T_DEV, :].astype(BF)


def finish(total, incoming):
    return pl.pallas_call(
        finish_kernel,
        out_shape=jax.ShapeDtypeStruct((T_DEV, STREAMS, D), BF),
        in_specs=whole(2),
        out_specs=pl.BlockSpec(memory_space=VMEM),
        compiler_params=params(),
        name="finish",
    )(total, incoming)


def solution(mesh):
    return jax.shard_map(
        body,
        mesh=mesh,
        in_specs=(
            P("expert", "dp", None),
            P("expert", "dp", None),
            P("expert", "dp", None),
            P("expert", "dp", None),
            P("expert", "dp", None),
            P("dp", None),
            P(("dp", "expert"), None),
            P(),
            P("expert", None, None),
            P("expert", None, None),
            P("expert", None, None),
            P("dp", "expert", None, None),
            P("dp", "expert", None, None),
        ),
        out_specs=P("expert", "dp", None),
        check_vma=False,
    )
```

```python
import functools

import jax
import jax.numpy as jnp
from jax import lax
from jax.experimental import pallas as pl
from jax.experimental.pallas import tpu as pltpu
from jax.sharding import PartitionSpec as P


HEADS = 16
NOPE = 128
ROPE = 64
V_DIM = 128
TOP = 6
EPSILON = 1e-06


N_DP = 8
N_X = 4
N_Y = 4
N_Z = 8
N_EXPERT = N_Y * N_Z
STREAMS = 2
T_DEV = 64
TOK = STREAMS * T_DEV
SLOTS = 36
PAIR = 2 * SLOTS
D = 2048
FF = 704
LENGTH = 2048
META = 8
BLOCK = TOK + META
VMEM = pltpu.MemorySpace.VMEM
BF = jnp.bfloat16
F32 = jnp.float32


def params(mib=40):
    return pltpu.CompilerParams(vmem_limit_bytes=mib << 20)


def whole(n):
    return [pl.BlockSpec(memory_space=VMEM) for _ in range(n)]


GROUP = 8


def pack_kernel(s, q_ref, k_ref, r_ref, v_ref, *rest):
    out_ref = rest[-1]
    rope = r_ref[:, s, :]
    for h in range(GROUP):
        at = h * (NOPE + ROPE)
        out_ref[0, h, 0:64, :] = q_ref[:, s, at : at + NOPE]
        out_ref[0, h, 64:128, :] = k_ref[:, s, h * NOPE : (h + 1) * NOPE]
        out_ref[0, h, 128:192, :] = v_ref[:, s, h * V_DIM : (h + 1) * V_DIM]
        out_ref[0, h, 192:256, :] = jnp.concatenate(
            [q_ref[:, s, at + NOPE : at + NOPE + ROPE], rope], axis=1
        )


def pack(s, first, steps, q, k, r, v, *part):
    wide = GROUP * (NOPE + ROPE)
    return pl.pallas_call(
        functools.partial(pack_kernel, s),
        grid=(steps,),
        out_shape=jax.ShapeDtypeStruct((STREAMS, HEADS, 256, 128), BF),
        in_specs=[
            pl.BlockSpec((T_DEV, STREAMS, wide), lambda i: (0, 0, first + i)),
            pl.BlockSpec((T_DEV, STREAMS, GROUP * NOPE), lambda i: (0, 0, first + i)),
            pl.BlockSpec((T_DEV, STREAMS, ROPE), lambda i: (0, 0, 0)),
            pl.BlockSpec((T_DEV, STREAMS, GROUP * V_DIM), lambda i: (0, 0, first + i)),
        ]
        + [pl.BlockSpec(memory_space=pl.ANY)] * len(part),
        out_specs=pl.BlockSpec((1, GROUP, 256, 128), lambda i: (s, first + i, 0, 0)),
        input_output_aliases={4: 0} if part else {},
        compiler_params=params(16),
        name="pack",
    )(q, k, r, v, *part)


QB = 256


def attend_kernel(split_ref, x_ref, o_ref, k_scr, v_scr):
    scale = (NOPE + ROPE) ** -0.5
    split = split_ref[0]
    log2e = 1.4426950408889634
    zero = jnp.zeros((T_DEV, ROPE), BF)
    for e in range(N_EXPERT):
        rows = slice(e * T_DEV, (e + 1) * T_DEV)
        k_scr[rows, 0:NOPE] = x_ref[e, 64:128, :]
        k_scr[rows, NOPE:256] = jnp.concatenate([x_ref[e, 192:256, 64:128], zero], axis=1)
        v_scr[rows, :] = x_ref[e, 128:192, :]
    per = QB // T_DEV
    for b in range(LENGTH // QB):
        n = (b + 1) * QB
        q = jnp.concatenate(
            [
                jnp.concatenate([x_ref[b * per + j, 0:64, :] for j in range(per)], axis=0),
                jnp.concatenate([x_ref[b * per + j, 192:256, :] for j in range(per)], axis=0),
            ],
            axis=1,
        )
        lane = lax.broadcasted_iota(jnp.int32, (QB, 256), 1)
        q = jnp.where(lane < NOPE + ROPE, q, jnp.zeros_like(q))
        scores = lax.dot_general(
            q, k_scr[0:n, :], (((1,), (1,)), ((), ())), preferred_element_type=F32
        )
        row = b * QB + lax.broadcasted_iota(jnp.int32, (QB, 1), 0)
        col = lax.broadcasted_iota(jnp.int32, (QB, n), 1)
        low = jnp.where(row >= split, split, 0)
        scores = jnp.where((col <= row) & (col >= low), scores, -1e30)
        peak = jnp.max(scores, axis=1, keepdims=True)
        raised = jnp.exp2((scores - peak) * (scale * log2e))
        total = jnp.sum(raised, axis=1, keepdims=True)
        mixed = jnp.dot(raised.astype(BF), v_scr[0:n, :], preferred_element_type=F32)
        mixed = (mixed / total).astype(BF)
        for j in range(per):
            o_ref[b * per + j] = mixed[j * T_DEV : (j + 1) * T_DEV, :]


def attend(split, x):
    return pl.pallas_call(
        attend_kernel,
        out_shape=jax.ShapeDtypeStruct((32, T_DEV, V_DIM), BF),
        in_specs=[pl.BlockSpec(memory_space=pltpu.MemorySpace.SMEM)] + whole(1),
        out_specs=pl.BlockSpec(memory_space=VMEM),
        scratch_shapes=[pltpu.VMEM((LENGTH, 256), BF), pltpu.VMEM((LENGTH, V_DIM), BF)],
        compiler_params=params(),
        name="attend",
    )(split, x)


PIECE = D // N_DP


def place_kernel(at_ref, *refs):
    pieces, out_ref = refs[:-1], refs[-1]
    n, rows = len(pieces), pieces[0].shape[0]
    for k, piece in enumerate(pieces):
        start = pl.multiple_of(lax.rem(at_ref[0] + (n - k), n) * rows, rows)
        out_ref[pl.ds(start, rows), :] = piece[...]


def unfold_kernel(at_ref, in_ref, out_ref):
    rows = in_ref.shape[0] // N_Z
    for k in range(N_Z):
        start = pl.multiple_of((at_ref[0] ^ k) * rows, rows)
        out_ref[pl.ds(start, rows), :] = in_ref[k * rows : (k + 1) * rows, :]


def unfold(at, x):
    return pl.pallas_call(
        unfold_kernel,
        out_shape=jax.ShapeDtypeStruct(x.shape, BF),
        in_specs=[pl.BlockSpec(memory_space=pltpu.MemorySpace.SMEM)] + whole(1),
        out_specs=pl.BlockSpec(memory_space=VMEM),
        compiler_params=params(16),
        name="unfold",
    )(at, x)


def place(at, pieces):
    rows = pieces[0].shape[0] * len(pieces)
    return pl.pallas_call(
        place_kernel,
        out_shape=jax.ShapeDtypeStruct((rows, D), BF),
        in_specs=[pl.BlockSpec(memory_space=pltpu.MemorySpace.SMEM)] + whole(len(pieces)),
        out_specs=pl.BlockSpec(memory_space=VMEM),
        compiler_params=params(16),
        name="place",
    )(at, *pieces)


def project_kernel(which_ref, x_ref, *refs):
    w_refs = refs[:10]
    res_ref, gain_ref, meta_ref, hid_ref, norm_ref = refs[10:]
    pieces = []
    for k, w_ref in enumerate(w_refs):
        first = which_ref[k]
        pieces.append(
            jnp.concatenate(
                [
                    jnp.concatenate(
                        [x_ref[s, first + j] for j in range(w_ref.shape[0] // V_DIM)], axis=1
                    )
                    for s in range(STREAMS)
                ],
                axis=0,
            )
        )
    square = jnp.zeros((TOK, 1), F32)
    for n in range(0, D, 256):
        cols = slice(n, n + 256)
        acc = jnp.concatenate([res_ref[:, s, cols] for s in range(STREAMS)], axis=0).astype(F32)
        for a, w_ref in zip(pieces, w_refs):
            acc = acc + jnp.dot(a, w_ref[:, cols], preferred_element_type=F32)
        hid_ref[:, cols] = acc
        square = square + jnp.sum(acc * acc, axis=1, keepdims=True)
    scale = lax.rsqrt(square / D + EPSILON)
    normed = hid_ref[...] * scale * gain_ref[...].astype(F32)
    norm_ref[0:TOK, :] = normed.astype(BF)
    norm_ref[TOK:BLOCK, :] = meta_ref[...]


def project(which, x, ws, res, gain, meta):
    return pl.pallas_call(
        project_kernel,
        out_shape=(
            jax.ShapeDtypeStruct((TOK, D), F32),
            jax.ShapeDtypeStruct((BLOCK, D), BF),
        ),
        in_specs=[pl.BlockSpec(memory_space=pltpu.MemorySpace.SMEM)] + whole(4 + len(ws)),
        out_specs=whole(2),
        compiler_params=params(),
        name="project",
    )(which, x.reshape(STREAMS, HEADS, T_DEV, V_DIM), *ws, res, gain, meta)


ALONE = 40
HALF = D // 2


def one_hot(meta, expert, slots):
    named = meta[:, 0:TOK].astype(F32)
    rows = lax.broadcasted_iota(jnp.int32, named.shape, 0)
    match = jnp.where((named == expert) & (rows < TOP), 1.0, 0.0)
    member = jnp.sum(match, axis=0, keepdims=True)
    token = lax.broadcasted_iota(jnp.int32, (TOK, TOK), 0)
    other = lax.broadcasted_iota(jnp.int32, (TOK, TOK), 1)
    before = jnp.where(token < other, 1.0, 0.0).astype(BF)
    rank = jnp.dot(
        jnp.broadcast_to(member, (8, TOK)).astype(BF), before, preferred_element_type=F32
    )[0:1, :]
    slot = lax.broadcasted_iota(jnp.int32, (slots, TOK), 0).astype(F32)
    return jnp.where((slot == rank) & (member > 0.5), 1.0, 0.0), match


def expert_at(at_ref, k):
    return (lax.rem(at_ref[0] + k, N_Y) * N_Z + at_ref[1]).astype(F32)


def select_two_kernel(at_ref, a_ref, b_ref, *outs):
    rows = jnp.concatenate([a_ref[0:TOK, :], b_ref[0:TOK, :]], axis=0)
    none = jnp.zeros((SLOTS, TOK), F32)
    picks = []
    for k in range(N_Y):
        hot_a, _ = one_hot(a_ref[TOK:BLOCK, :], expert_at(at_ref, k), SLOTS)
        hot_b, _ = one_hot(b_ref[TOK:BLOCK, :], expert_at(at_ref, k), SLOTS)
        picks += [jnp.concatenate([hot_a, none], axis=1), jnp.concatenate([none, hot_b], axis=1)]
    picks = jnp.concatenate(picks, axis=0).astype(BF)
    chosen = jnp.dot(picks, rows, preferred_element_type=F32).astype(BF)
    for k in range(N_Y):
        outs[k][...] = chosen[k * PAIR : (k + 1) * PAIR, :]


def select_one_kernel(at_ref, *refs):
    parts, outs = refs[:-N_Y], refs[-N_Y:]
    meta = parts[0][TOK:BLOCK, :]
    picks = [one_hot(meta, expert_at(at_ref, k), ALONE)[0] for k in range(N_Y)]
    picks = jnp.concatenate(picks, axis=0).astype(BF)
    start = 0
    for part in parts:
        wide = part.shape[1]
        chosen = jnp.dot(picks, part[0:TOK, :], preferred_element_type=F32).astype(BF)
        for k in range(N_Y):
            outs[k][:, start : start + wide] = chosen[k * ALONE : (k + 1) * ALONE, :]
        start += wide


def select(at, parts, alone):
    return pl.pallas_call(
        select_one_kernel if alone else select_two_kernel,
        out_shape=[jax.ShapeDtypeStruct((ALONE if alone else PAIR, D), BF)] * N_Y,
        in_specs=[pl.BlockSpec(memory_space=pltpu.MemorySpace.SMEM)] + whole(len(parts)),
        out_specs=whole(N_Y),
        compiler_params=params(),
        name="select",
    )(at, *parts)


EK = 512


def expert_kernel(n, *refs):
    xs, (gate_ref, up_ref, down_ref) = refs[:n], refs[n : n + 3]
    ys, (g_scr, u_scr) = refs[n + 3 : 2 * n + 3], refs[2 * n + 3 :]
    step = pl.program_id(0)
    rows = jnp.concatenate([x[...] for x in xs], axis=0)
    across = (((1,), (1,)), ((), ()))
    g = lax.dot_general(rows, gate_ref[0], across, preferred_element_type=F32)
    u = lax.dot_general(rows, up_ref[0], across, preferred_element_type=F32)

    @pl.when(step == 0)
    def _():
        g_scr[...] = g
        u_scr[...] = u

    @pl.when(step > 0)
    def _():
        g_scr[...] += g
        u_scr[...] += u

    @pl.when(step == pl.num_programs(0) - 1)
    def _():
        gate = g_scr[...]
        act = (gate / (1.0 + jnp.exp(-gate)) * u_scr[...]).astype(BF)
        out = jnp.dot(act, down_ref[0], preferred_element_type=F32).astype(BF)
        start = 0
        for y in ys:
            y[...] = out[start : start + y.shape[0], :]
            start += y.shape[0]


def expert(xs, gate, up, down):
    n = len(xs)
    total = sum(x.shape[0] for x in xs)
    return pl.pallas_call(
        functools.partial(expert_kernel, n),
        grid=(D // EK,),
        out_shape=[jax.ShapeDtypeStruct(x.shape, BF) for x in xs],
        in_specs=[pl.BlockSpec((x.shape[0], EK), lambda i: (0, i)) for x in xs]
        + [
            pl.BlockSpec((1, FF, EK), lambda i: (0, 0, i)),
            pl.BlockSpec((1, FF, EK), lambda i: (0, 0, i)),
            pl.BlockSpec((1, FF, D), lambda i: (0, 0, 0)),
        ],
        out_specs=[pl.BlockSpec(x.shape, lambda i: (0, 0)) for x in xs],
        scratch_shapes=[pltpu.VMEM((total, FF), F32), pltpu.VMEM((total, FF), F32)],
        compiler_params=params(),
        name="expert",
    )(*xs, gate, up, down)


def weighted(at_ref, meta, slots, first, height, rows):
    high = meta[:, TOK : 2 * TOK].astype(F32)
    low = meta[:, 2 * TOK : 3 * TOK].astype(F32)
    highs, lows = [], []
    before, after = first, height - first - slots
    for k in range(N_Y):
        hot, match = one_hot(meta, expert_at(at_ref, k), slots)
        for scale, into in ((high, highs), (low, lows)):
            if before:
                into.append(jnp.zeros((before, TOK), F32))
            into.append(hot * jnp.sum(match * scale, axis=0, keepdims=True))
            if after:
                into.append(jnp.zeros((after, TOK), F32))
    contract = (((0,), (0,)), ((), ()))
    return sum(
        lax.dot_general(
            jnp.concatenate(w, axis=0).astype(BF), rows, contract, preferred_element_type=F32
        )
        for w in (highs, lows)
    )


def far_kernel(at_ref, meta_ref, r0, r1, r2, r3, left_ref, right_ref):
    rows = jnp.concatenate([r[...] for r in (r0, r1, r2, r3)], axis=0)
    total = weighted(at_ref, meta_ref[...], ALONE, 0, ALONE, rows).astype(BF)
    left_ref[...] = total[:, :HALF]
    right_ref[...] = total[:, HALF:]


def two_kernel(at_ref, a_ref, b_ref, r0, r1, r2, r3, out_a, out_b):
    rows = jnp.concatenate([r[...] for r in (r0, r1, r2, r3)], axis=0)
    out_a[...] = weighted(at_ref, a_ref[...], SLOTS, 0, PAIR, rows)
    out_b[...] = weighted(at_ref, b_ref[...], SLOTS, SLOTS, PAIR, rows)


def own_kernel(at_ref, meta_ref, r0, r1, r2, r3, hid_ref, out_ref):
    rows = jnp.concatenate([r[...] for r in (r0, r1, r2, r3)], axis=0)
    out_ref[...] = hid_ref[...] + weighted(at_ref, meta_ref[...], ALONE, 0, ALONE, rows)


def sums(kernel, at, blocks, rets, extra, shapes):
    def flat(x):
        return pl.BlockSpec(x.shape, lambda i: (0, 0))

    metas = [pl.BlockSpec((META, b.shape[1]), lambda i: (TOK // META, 0)) for b in blocks]
    return pl.pallas_call(
        kernel,
        grid=(1,),
        out_shape=shapes,
        in_specs=[pl.BlockSpec(memory_space=pltpu.MemorySpace.SMEM)]
        + metas
        + [flat(x) for x in (*rets, *extra)],
        out_specs=[flat(x) for x in shapes],
        compiler_params=params(),
        name="sums",
    )(at, *blocks, *rets, *extra)


def join_kernel(pa_ref, pb_ref, a_ref, b_ref, out_a, out_b):
    if a_ref.shape[1] == D:
        out_a[...] = (pa_ref[...] + a_ref[...].astype(F32)).astype(BF)
        out_b[...] = (pb_ref[...] + b_ref[...].astype(F32)).astype(BF)
    else:
        out_a[:, :HALF] = pa_ref[:, :HALF].astype(BF)
        out_a[:, HALF:] = (pa_ref[:, HALF:] + a_ref[...].astype(F32)).astype(BF)
        out_b[:, :HALF] = (pb_ref[:, :HALF] + b_ref[...].astype(F32)).astype(BF)
        out_b[:, HALF:] = pb_ref[:, HALF:].astype(BF)


def join(pa, pb, a, b):
    return pl.pallas_call(
        join_kernel,
        out_shape=[jax.ShapeDtypeStruct((TOK, D), BF)] * 2,
        in_specs=whole(4),
        out_specs=whole(2),
        compiler_params=params(16),
        name="join",
    )(pa, pb, a, b)


def finish_kernel(own_ref, a_ref, b_ref, out_ref):
    total = own_ref[...] + a_ref[...].astype(F32) + b_ref[...].astype(F32)
    for s in range(STREAMS):
        out_ref[:, s, :] = total[s * T_DEV : (s + 1) * T_DEV, :].astype(BF)


def finish(own, a, b):
    return pl.pallas_call(
        finish_kernel,
        out_shape=jax.ShapeDtypeStruct((T_DEV, STREAMS, D), BF),
        in_specs=whole(3),
        out_specs=pl.BlockSpec(memory_space=VMEM),
        compiler_params=params(16),
        name="finish",
    )(own, a, b)


def along_z(x, k):
    pairs = [(y * N_Z + z, y * N_Z + (z + k) % N_Z) for y in range(N_Y) for z in range(N_Z)]
    return lax.ppermute(x, "expert", pairs)


def along_y(x, k):
    pairs = [(y * N_Z + z, (y + k) % N_Y * N_Z + z) for y in range(N_Y) for z in range(N_Z)]
    return lax.ppermute(x, "expert", pairs)


def across_z(x, bit):
    pairs = [(y * N_Z + z, y * N_Z + (z ^ bit)) for y in range(N_Y) for z in range(N_Z)]
    return lax.ppermute(x, "expert", pairs)


def along_dp(x, hops, swap):
    pairs = [
        (p * 2 + c, (p + hops) % N_X * 2 + (c + swap) % 2) for p in range(N_X) for c in range(2)
    ]
    return lax.ppermute(x, "dp", pairs)


def meta_rows(routes, route_weights):
    ids = routes.reshape(T_DEV, STREAMS, TOP).transpose(2, 1, 0).reshape(TOP, TOK)
    scales = route_weights.reshape(T_DEV, STREAMS, TOP).transpose(2, 1, 0).reshape(TOP, TOK)
    high = lax.reduce_precision(scales, 8, 7)
    both = jnp.concatenate([ids.astype(F32), high, scales - high], axis=1)
    return jnp.pad(both, ((0, META - TOP), (0, D - 3 * TOK))).astype(BF)


def body(
    queries,
    key_nope,
    key_rope,
    values,
    residual,
    segments,
    out_proj,
    norm_gain,
    expert_gate,
    expert_up,
    expert_down,
    routes,
    route_weights,
):
    me = lax.axis_index("expert")
    at = jnp.stack([me // N_Z, me % N_Z]).astype(jnp.int32)
    meta = meta_rows(routes, route_weights)

    inputs = (queries, key_nope, key_rope, values)
    slab = jnp.concatenate([out_proj, across_z(out_proj, 1)], axis=0)
    sent = pack(0, 0, 2, *inputs)
    slab = jnp.concatenate([slab, across_z(slab, 2)], axis=0)
    sent = pack(1, 0, 1, *inputs, sent)
    slab = jnp.concatenate([slab, across_z(slab, 4)], axis=0)
    sent = pack(1, 1, 1, *inputs, sent)
    got = lax.all_to_all(sent.reshape(N_EXPERT, 256, 128), "expert", 0, 0, tiled=True)
    slab = unfold(at[1:2], slab)
    slabs = [slab] + [along_y(slab, k) for k in range(1, N_Y)]
    slab = place(at[0:1], slabs)
    up1, down1 = along_dp(slab, 1, 0), along_dp(slab, -1, 0)
    cut = PIECE // 2
    far = (along_dp(up1[:cut], 1, 0), along_dp(down1[cut:], -1, 0))
    pieces = [slab, up1, down1, *far]
    pieces += [along_dp(w, 0, 1) for w in pieces]
    dp = lax.axis_index("dp")
    x, core = dp // 2, dp % 2
    heads = PIECE // V_DIM
    which = jnp.stack(
        [
            ((x + n) % N_X * 2 + (core + c) % 2) * heads + more
            for c in range(2)
            for n, more in ((0, 0), (3, 0), (1, 0), (2, 0), (2, heads // 2))
        ]
    ).astype(jnp.int32)

    stream = me // HEADS
    ones = jnp.sum(segments, axis=1)
    split = LENGTH - jnp.where(stream == 0, ones[0], ones[1])
    mixed = attend(split.reshape(1), got)
    back = lax.all_to_all(mixed, "expert", 0, 0, tiled=True)
    hidden, own = project(which, back, pieces, residual, norm_gain.reshape(1, D), meta)
    weights = (jnp.swapaxes(expert_gate, 1, 2), jnp.swapaxes(expert_up, 1, 2), expert_down)

    def to_experts(parts, alone):
        rows = select(at, parts, alone)
        return [rows[0]] + [along_y(rows[k], k) for k in range(1, N_Y)]

    def to_tokens(ys):
        return [ys[0]] + [along_y(ys[k], -k) for k in range(1, N_Y)]

    right, left = [own], [own]
    xs = [to_experts([own], True)]
    for k in range(1, 4):
        right.append(along_z(right[-1], 1))
        left.append(along_z(left[-1], -1))
        xs.append(to_experts([left[k], right[k]], False))
    ends = [along_z(right[3][:, :HALF], 1), along_z(left[3][:, HALF:], -1)]
    xs.append(to_experts(ends, True))

    ys = [None] * 5
    for n in range(5):
        ys[n] = expert(xs[n], *weights)
    rets = [to_tokens(ys[n]) for n in range(5)]

    halves = [jax.ShapeDtypeStruct((TOK, HALF), BF)] * 2
    down, up = sums(far_kernel, at, [ends[0]], rets[4], (), halves)
    for k in (3, 2, 1):
        full = [jax.ShapeDtypeStruct((TOK, D), F32)] * 2
        to_up, to_down = sums(two_kernel, at, [left[k], right[k]], rets[k], (), full)
        up, down = along_z(up, 1), along_z(down, -1)
        up, down = join(to_up, to_down, up, down)
    alone = [jax.ShapeDtypeStruct((TOK, D), F32)]
    (total,) = sums(own_kernel, at, [own], rets[0], (hidden,), alone)
    return finish(total, along_z(up, 1), along_z(down, -1))


def solution(mesh):
    return jax.shard_map(
        body,
        mesh=mesh,
        in_specs=(
            P("expert", "dp", None),
            P("expert", "dp", None),
            P("expert", "dp", None),
            P("expert", "dp", None),
            P("expert", "dp", None),
            P("dp", None),
            P(("dp", "expert"), None),
            P(),
            P("expert", None, None),
            P("expert", None, None),
            P("expert", None, None),
            P("dp", "expert", None, None),
            P("dp", "expert", None, None),
        ),
        out_specs=P("expert", "dp", None),
        check_vma=False,
    )
```

```python
import functools

import jax
import jax.numpy as jnp
from jax import lax
from jax.experimental import pallas as pl
from jax.experimental.pallas import tpu as pltpu
from jax.sharding import PartitionSpec as P


HEADS = 16
NOPE = 128
ROPE = 64
V_DIM = 128
TOP = 6
EPSILON = 1e-06


N_DP = 8
N_X = 4
N_Y = 4
N_Z = 8
N_EXPERT = N_Y * N_Z
STREAMS = 2
T_DEV = 64
TOK = STREAMS * T_DEV
SLOTS = 36
PAIR = 2 * SLOTS
D = 2048
FF = 704
LENGTH = 2048
HALF = D // 2
META = 8
BLOCK = TOK + META
VMEM = pltpu.MemorySpace.VMEM
BF = jnp.bfloat16
F32 = jnp.float32


def params(mib=40):
    return pltpu.CompilerParams(vmem_limit_bytes=mib << 20)


def whole(n):
    return [pl.BlockSpec(memory_space=VMEM) for _ in range(n)]


GROUP = 8


def pack_kernel(s, q_ref, k_ref, r_ref, v_ref, *rest):
    out_ref = rest[-1]
    rope = r_ref[:, s, :]
    for h in range(GROUP):
        at = h * (NOPE + ROPE)
        out_ref[0, h, 0:64, :] = q_ref[:, s, at : at + NOPE]
        out_ref[0, h, 64:128, :] = k_ref[:, s, h * NOPE : (h + 1) * NOPE]
        out_ref[0, h, 128:192, :] = v_ref[:, s, h * V_DIM : (h + 1) * V_DIM]
        out_ref[0, h, 192:256, :] = jnp.concatenate(
            [q_ref[:, s, at + NOPE : at + NOPE + ROPE], rope], axis=1
        )


def pack(s, first, steps, q, k, r, v, *part):
    wide = GROUP * (NOPE + ROPE)
    return pl.pallas_call(
        functools.partial(pack_kernel, s),
        grid=(steps,),
        out_shape=jax.ShapeDtypeStruct((STREAMS, HEADS, 256, 128), BF),
        in_specs=[
            pl.BlockSpec((T_DEV, STREAMS, wide), lambda i: (0, 0, first + i)),
            pl.BlockSpec((T_DEV, STREAMS, GROUP * NOPE), lambda i: (0, 0, first + i)),
            pl.BlockSpec((T_DEV, STREAMS, ROPE), lambda i: (0, 0, 0)),
            pl.BlockSpec((T_DEV, STREAMS, GROUP * V_DIM), lambda i: (0, 0, first + i)),
        ]
        + [pl.BlockSpec(memory_space=pl.ANY)] * len(part),
        out_specs=pl.BlockSpec((1, GROUP, 256, 128), lambda i: (s, first + i, 0, 0)),
        input_output_aliases={4: 0} if part else {},
        compiler_params=params(16),
        name="pack",
    )(q, k, r, v, *part)


QB = 256


def attend_kernel(split_ref, x_ref, o_ref, k_scr, v_scr):
    scale = (NOPE + ROPE) ** -0.5
    split = split_ref[0]
    log2e = 1.4426950408889634
    zero = jnp.zeros((T_DEV, ROPE), BF)
    for e in range(N_EXPERT):
        rows = slice(e * T_DEV, (e + 1) * T_DEV)
        k_scr[rows, 0:NOPE] = x_ref[e, 64:128, :]
        k_scr[rows, NOPE:256] = jnp.concatenate([x_ref[e, 192:256, 64:128], zero], axis=1)
        v_scr[rows, :] = x_ref[e, 128:192, :]
    per = QB // T_DEV
    for b in range(LENGTH // QB):
        n = (b + 1) * QB
        q = jnp.concatenate(
            [
                jnp.concatenate([x_ref[b * per + j, 0:64, :] for j in range(per)], axis=0),
                jnp.concatenate([x_ref[b * per + j, 192:256, :] for j in range(per)], axis=0),
            ],
            axis=1,
        )
        lane = lax.broadcasted_iota(jnp.int32, (QB, 256), 1)
        q = jnp.where(lane < NOPE + ROPE, q, jnp.zeros_like(q))
        scores = lax.dot_general(
            q, k_scr[0:n, :], (((1,), (1,)), ((), ())), preferred_element_type=F32
        )
        row = b * QB + lax.broadcasted_iota(jnp.int32, (QB, 1), 0)
        col = lax.broadcasted_iota(jnp.int32, (QB, n), 1)
        low = jnp.where(row >= split, split, 0)
        scores = jnp.where((col <= row) & (col >= low), scores, -1e30)
        peak = jnp.max(scores, axis=1, keepdims=True)
        raised = jnp.exp2((scores - peak) * (scale * log2e))
        total = jnp.sum(raised, axis=1, keepdims=True)
        mixed = jnp.dot(raised.astype(BF), v_scr[0:n, :], preferred_element_type=F32)
        mixed = (mixed / total).astype(BF)
        for j in range(per):
            o_ref[b * per + j] = mixed[j * T_DEV : (j + 1) * T_DEV, :]


def attend(split, x):
    return pl.pallas_call(
        attend_kernel,
        out_shape=jax.ShapeDtypeStruct((32, T_DEV, V_DIM), BF),
        in_specs=[pl.BlockSpec(memory_space=pltpu.MemorySpace.SMEM)] + whole(1),
        out_specs=pl.BlockSpec(memory_space=VMEM),
        scratch_shapes=[pltpu.VMEM((LENGTH, 256), BF), pltpu.VMEM((LENGTH, V_DIM), BF)],
        compiler_params=params(),
        name="attend",
    )(split, x)


PIECE = D // N_DP


def place_kernel(at_ref, *refs):
    pieces, out_ref = refs[:-1], refs[-1]
    n, rows = len(pieces), pieces[0].shape[0]
    for k, piece in enumerate(pieces):
        start = pl.multiple_of(lax.rem(at_ref[0] + (n - k), n) * rows, rows)
        out_ref[pl.ds(start, rows), :] = piece[...]


def unfold_kernel(at_ref, in_ref, out_ref):
    rows = in_ref.shape[0] // N_Z
    for k in range(N_Z):
        apart = (k & 1) * 4 + (k & 2) + (k >> 2)
        start = pl.multiple_of((at_ref[0] ^ apart) * rows, rows)
        out_ref[pl.ds(start, rows), :] = in_ref[k * rows : (k + 1) * rows, :]


def unfold(at, x):
    return pl.pallas_call(
        unfold_kernel,
        out_shape=jax.ShapeDtypeStruct(x.shape, BF),
        in_specs=[pl.BlockSpec(memory_space=pltpu.MemorySpace.SMEM)] + whole(1),
        out_specs=pl.BlockSpec(memory_space=VMEM),
        compiler_params=params(16),
        name="unfold",
    )(at, x)


def place(at, pieces):
    rows = pieces[0].shape[0] * len(pieces)
    return pl.pallas_call(
        place_kernel,
        out_shape=jax.ShapeDtypeStruct((rows, D), BF),
        in_specs=[pl.BlockSpec(memory_space=pltpu.MemorySpace.SMEM)] + whole(len(pieces)),
        out_specs=pl.BlockSpec(memory_space=VMEM),
        compiler_params=params(16),
        name="place",
    )(at, *pieces)


def project_kernel(which_ref, x_ref, *refs):
    w_refs = refs[:10]
    res_ref, gain_ref, meta_ref, hid_ref, near_ref, away_ref = refs[10:]
    pieces = []
    for k, w_ref in enumerate(w_refs):
        first = which_ref[k]
        pieces.append(
            jnp.concatenate(
                [
                    jnp.concatenate(
                        [x_ref[s, first + j] for j in range(w_ref.shape[0] // V_DIM)], axis=1
                    )
                    for s in range(STREAMS)
                ],
                axis=0,
            )
        )
    square = jnp.zeros((TOK, 1), F32)
    for n in range(0, D, 256):
        cols = slice(n, n + 256)
        acc = jnp.concatenate([res_ref[:, s, cols] for s in range(STREAMS)], axis=0).astype(F32)
        for a, w_ref in zip(pieces, w_refs):
            acc = acc + jnp.dot(a, w_ref[:, cols], preferred_element_type=F32)
        hid_ref[:, cols] = acc
        square = square + jnp.sum(acc * acc, axis=1, keepdims=True)
    scale = lax.rsqrt(square / D + EPSILON)
    for n, out_ref in ((0, near_ref), (HALF, away_ref)):
        cols = slice(n, n + HALF)
        normed = hid_ref[:, cols] * scale * gain_ref[:, cols].astype(F32)
        out_ref[0:TOK, :] = normed.astype(BF)
    near_ref[TOK:BLOCK, :] = meta_ref[...]


def project(which, x, ws, res, gain, meta):
    return pl.pallas_call(
        project_kernel,
        out_shape=(
            jax.ShapeDtypeStruct((TOK, D), F32),
            jax.ShapeDtypeStruct((BLOCK, HALF), BF),
            jax.ShapeDtypeStruct((TOK, HALF), BF),
        ),
        in_specs=[pl.BlockSpec(memory_space=pltpu.MemorySpace.SMEM)] + whole(4 + len(ws)),
        out_specs=whole(3),
        compiler_params=params(),
        name="project",
    )(which, x.reshape(STREAMS, HEADS, T_DEV, V_DIM), *ws, res, gain, meta)


ALONE = 40


def one_hot(meta, expert, slots):
    named = meta[:, 0:TOK].astype(F32)
    rows = lax.broadcasted_iota(jnp.int32, named.shape, 0)
    match = jnp.where((named == expert) & (rows < TOP), 1.0, 0.0)
    member = jnp.sum(match, axis=0, keepdims=True)
    token = lax.broadcasted_iota(jnp.int32, (TOK, TOK), 0)
    other = lax.broadcasted_iota(jnp.int32, (TOK, TOK), 1)
    before = jnp.where(token < other, 1.0, 0.0).astype(BF)
    rank = jnp.dot(
        jnp.broadcast_to(member, (8, TOK)).astype(BF), before, preferred_element_type=F32
    )[0:1, :]
    slot = lax.broadcasted_iota(jnp.int32, (slots, TOK), 0).astype(F32)
    return jnp.where((slot == rank) & (member > 0.5), 1.0, 0.0), match


def expert_at(at_ref, k):
    return (lax.rem(at_ref[0] + k, N_Y) * N_Z + at_ref[1]).astype(F32)


def select_two_kernel(at_ref, a_ref, a_rest, b_ref, b_rest, *outs):
    none = jnp.zeros((SLOTS, TOK), F32)
    picks = []
    for k in range(N_Y):
        hot_a, _ = one_hot(a_ref[TOK:BLOCK, :], expert_at(at_ref, k), SLOTS)
        hot_b, _ = one_hot(b_ref[TOK:BLOCK, :], expert_at(at_ref, k), SLOTS)
        picks += [jnp.concatenate([hot_a, none], axis=1), jnp.concatenate([none, hot_b], axis=1)]
    picks = jnp.concatenate(picks, axis=0).astype(BF)
    for n, a, b in ((0, a_ref, b_ref), (HALF, a_rest, b_rest)):
        rows = jnp.concatenate([a[0:TOK, :], b[0:TOK, :]], axis=0)
        chosen = jnp.dot(picks, rows, preferred_element_type=F32).astype(BF)
        for k in range(N_Y):
            outs[k][:, n : n + HALF] = chosen[k * PAIR : (k + 1) * PAIR, :]


def select_one_kernel(at_ref, *refs):
    parts, outs = refs[:-N_Y], refs[-N_Y:]
    meta = parts[0][TOK:BLOCK, :]
    picks = [one_hot(meta, expert_at(at_ref, k), ALONE)[0] for k in range(N_Y)]
    picks = jnp.concatenate(picks, axis=0).astype(BF)
    start = 0
    for part in parts:
        wide = part.shape[1]
        chosen = jnp.dot(picks, part[0:TOK, :], preferred_element_type=F32).astype(BF)
        for k in range(N_Y):
            outs[k][:, start : start + wide] = chosen[k * ALONE : (k + 1) * ALONE, :]
        start += wide


def select(at, parts, alone):
    return pl.pallas_call(
        select_one_kernel if alone else select_two_kernel,
        out_shape=[jax.ShapeDtypeStruct((ALONE if alone else PAIR, D), BF)] * N_Y,
        in_specs=[pl.BlockSpec(memory_space=pltpu.MemorySpace.SMEM)] + whole(len(parts)),
        out_specs=whole(N_Y),
        compiler_params=params(),
        name="select",
    )(at, *parts)


EK = 512


def expert_kernel(n, *refs):
    xs, (gate_ref, up_ref, down_ref) = refs[:n], refs[n : n + 3]
    ys, (g_scr, u_scr) = refs[n + 3 : 2 * n + 3], refs[2 * n + 3 :]
    step = pl.program_id(0)
    rows = jnp.concatenate([x[...] for x in xs], axis=0)
    across = (((1,), (1,)), ((), ()))
    g = lax.dot_general(rows, gate_ref[0], across, preferred_element_type=F32)
    u = lax.dot_general(rows, up_ref[0], across, preferred_element_type=F32)

    @pl.when(step == 0)
    def _():
        g_scr[...] = g
        u_scr[...] = u

    @pl.when(step > 0)
    def _():
        g_scr[...] += g
        u_scr[...] += u

    @pl.when(step == pl.num_programs(0) - 1)
    def _():
        gate = g_scr[...]
        act = (gate / (1.0 + jnp.exp(-gate)) * u_scr[...]).astype(BF)
        out = jnp.dot(act, down_ref[0], preferred_element_type=F32).astype(BF)
        start = 0
        for y in ys:
            y[...] = out[start : start + y.shape[0], :]
            start += y.shape[0]


def expert(xs, gate, up, down):
    n = len(xs)
    total = sum(x.shape[0] for x in xs)
    return pl.pallas_call(
        functools.partial(expert_kernel, n),
        grid=(D // EK,),
        out_shape=[jax.ShapeDtypeStruct(x.shape, BF) for x in xs],
        in_specs=[pl.BlockSpec((x.shape[0], EK), lambda i: (0, i)) for x in xs]
        + [
            pl.BlockSpec((1, FF, EK), lambda i: (0, 0, i)),
            pl.BlockSpec((1, FF, EK), lambda i: (0, 0, i)),
            pl.BlockSpec((1, FF, D), lambda i: (0, 0, 0)),
        ],
        out_specs=[pl.BlockSpec(x.shape, lambda i: (0, 0)) for x in xs],
        scratch_shapes=[pltpu.VMEM((total, FF), F32), pltpu.VMEM((total, FF), F32)],
        compiler_params=params(),
        name="expert",
    )(*xs, gate, up, down)


def weighted(at_ref, meta, slots, first, height, rows):
    high = meta[:, TOK : 2 * TOK].astype(F32)
    low = meta[:, 2 * TOK : 3 * TOK].astype(F32)
    highs, lows = [], []
    before, after = first, height - first - slots
    for k in range(N_Y):
        hot, match = one_hot(meta, expert_at(at_ref, k), slots)
        for scale, into in ((high, highs), (low, lows)):
            if before:
                into.append(jnp.zeros((before, TOK), F32))
            into.append(hot * jnp.sum(match * scale, axis=0, keepdims=True))
            if after:
                into.append(jnp.zeros((after, TOK), F32))
    contract = (((0,), (0,)), ((), ()))
    return sum(
        lax.dot_general(
            jnp.concatenate(w, axis=0).astype(BF), rows, contract, preferred_element_type=F32
        )
        for w in (highs, lows)
    )


def far_kernel(at_ref, meta_ref, r0, r1, r2, r3, down_ref, up_ref):
    rows = jnp.concatenate([r[...] for r in (r0, r1, r2, r3)], axis=0)
    total = weighted(at_ref, meta_ref[...], ALONE, 0, ALONE, rows).astype(BF)
    down_ref[...] = total[:, :HALF]
    up_ref[...] = total[:, HALF:]


def two_kernel(at_ref, a_ref, b_ref, r0, r1, r2, r3, up_0, up_1, down_0, down_1):
    rows = jnp.concatenate([r[...] for r in (r0, r1, r2, r3)], axis=0)
    up = weighted(at_ref, a_ref[...], SLOTS, 0, PAIR, rows)
    up_0[...] = up[:, :HALF].astype(up_0.dtype)
    up_1[...] = up[:, HALF:]
    down = weighted(at_ref, b_ref[...], SLOTS, SLOTS, PAIR, rows)
    down_0[...] = down[:, :HALF]
    down_1[...] = down[:, HALF:].astype(down_1.dtype)


def own_kernel(at_ref, meta_ref, r0, r1, r2, r3, hid_ref, out_ref):
    rows = jnp.concatenate([r[...] for r in (r0, r1, r2, r3)], axis=0)
    out_ref[...] = hid_ref[...] + weighted(at_ref, meta_ref[...], ALONE, 0, ALONE, rows)


def sums(kernel, at, blocks, rets, extra, shapes):
    def flat(x):
        return pl.BlockSpec(x.shape, lambda i: (0, 0))

    metas = [pl.BlockSpec((META, b.shape[1]), lambda i: (TOK // META, 0)) for b in blocks]
    return pl.pallas_call(
        kernel,
        grid=(1,),
        out_shape=shapes,
        in_specs=[pl.BlockSpec(memory_space=pltpu.MemorySpace.SMEM)]
        + metas
        + [flat(x) for x in (*rets, *extra)],
        out_specs=[flat(x) for x in shapes],
        compiler_params=params(),
        name="sums",
    )(at, *blocks, *rets, *extra)


def join_kernel(pa_ref, pb_ref, a_ref, b_ref, out_a, out_b):
    out_a[...] = (pa_ref[...] + a_ref[...].astype(F32)).astype(BF)
    out_b[...] = (pb_ref[...] + b_ref[...].astype(F32)).astype(BF)


def join(pa, pb, a, b):
    return pl.pallas_call(
        join_kernel,
        out_shape=[jax.ShapeDtypeStruct((TOK, HALF), BF)] * 2,
        in_specs=whole(4),
        out_specs=whole(2),
        compiler_params=params(16),
        name="join",
    )(pa, pb, a, b)


def finish_kernel(own_ref, up_0, up_1, down_0, down_1, out_ref):
    for n, up, down in ((0, up_0, down_0), (HALF, up_1, down_1)):
        cols = slice(n, n + HALF)
        total = own_ref[:, cols] + up[...].astype(F32) + down[...].astype(F32)
        for s in range(STREAMS):
            out_ref[:, s, cols] = total[s * T_DEV : (s + 1) * T_DEV, :].astype(BF)


def finish(own, *halves):
    return pl.pallas_call(
        finish_kernel,
        out_shape=jax.ShapeDtypeStruct((T_DEV, STREAMS, D), BF),
        in_specs=whole(5),
        out_specs=pl.BlockSpec(memory_space=VMEM),
        compiler_params=params(16),
        name="finish",
    )(own, *halves)


def along_z(x, k):
    pairs = [(y * N_Z + z, y * N_Z + (z + k) % N_Z) for y in range(N_Y) for z in range(N_Z)]
    return lax.ppermute(x, "expert", pairs)


def along_y(x, k):
    pairs = [(y * N_Z + z, (y + k) % N_Y * N_Z + z) for y in range(N_Y) for z in range(N_Z)]
    return lax.ppermute(x, "expert", pairs)


def across_z(x, bit):
    pairs = [(y * N_Z + z, y * N_Z + (z ^ bit)) for y in range(N_Y) for z in range(N_Z)]
    return lax.ppermute(x, "expert", pairs)


def along_dp(x, hops, swap):
    pairs = [
        (p * 2 + c, (p + hops) % N_X * 2 + (c + swap) % 2) for p in range(N_X) for c in range(2)
    ]
    return lax.ppermute(x, "dp", pairs)


def meta_rows(routes, route_weights):
    ids = routes.reshape(T_DEV, STREAMS, TOP).transpose(2, 1, 0).reshape(TOP, TOK)
    scales = route_weights.reshape(T_DEV, STREAMS, TOP).transpose(2, 1, 0).reshape(TOP, TOK)
    high = lax.reduce_precision(scales, 8, 7)
    both = jnp.concatenate([ids.astype(F32), high, scales - high], axis=1)
    return jnp.pad(both, ((0, META - TOP), (0, HALF - 3 * TOK))).astype(BF)


def body(
    queries,
    key_nope,
    key_rope,
    values,
    residual,
    segments,
    out_proj,
    norm_gain,
    expert_gate,
    expert_up,
    expert_down,
    routes,
    route_weights,
):
    me = lax.axis_index("expert")
    at = jnp.stack([me // N_Z, me % N_Z]).astype(jnp.int32)
    meta = meta_rows(routes, route_weights)

    inputs = (queries, key_nope, key_rope, values)
    slab = jnp.concatenate([out_proj, across_z(out_proj, 4)], axis=0)
    sent = pack(0, 0, 2, *inputs)
    slab = jnp.concatenate([slab, across_z(slab, 2)], axis=0)
    sent = pack(1, 0, 1, *inputs, sent)
    slab = jnp.concatenate([slab, across_z(slab, 1)], axis=0)
    sent = pack(1, 1, 1, *inputs, sent)
    got = lax.all_to_all(sent.reshape(N_EXPERT, 256, 128), "expert", 0, 0, tiled=True)
    slab = unfold(at[1:2], slab)
    slabs = [slab] + [along_y(slab, k) for k in range(1, N_Y)]
    slab = place(at[0:1], slabs)
    up1, down1 = along_dp(slab, 1, 0), along_dp(slab, -1, 0)
    cut = PIECE // 2
    far = (along_dp(up1[:cut], 1, 0), along_dp(down1[cut:], -1, 0))
    pieces = [slab, up1, down1, *far]
    pieces += [along_dp(w, 0, 1) for w in pieces]
    dp = lax.axis_index("dp")
    x, core = dp // 2, dp % 2
    heads = PIECE // V_DIM
    which = jnp.stack(
        [
            ((x + n) % N_X * 2 + (core + c) % 2) * heads + more
            for c in range(2)
            for n, more in ((0, 0), (3, 0), (1, 0), (2, 0), (2, heads // 2))
        ]
    ).astype(jnp.int32)

    stream = me // HEADS
    ones = jnp.sum(segments, axis=1)
    split = LENGTH - jnp.where(stream == 0, ones[0], ones[1])
    mixed = attend(split.reshape(1), got)
    back = lax.all_to_all(mixed, "expert", 0, 0, tiled=True)
    hidden, *own = project(which, back, pieces, residual, norm_gain.reshape(1, D), meta)
    weights = (jnp.swapaxes(expert_gate, 1, 2), jnp.swapaxes(expert_up, 1, 2), expert_down)

    def to_experts(parts, alone):
        rows = select(at, parts, alone)
        return [rows[0]] + [along_y(rows[k], k) for k in range(1, N_Y)]

    def to_tokens(ys):
        return [ys[0]] + [along_y(ys[k], -k) for k in range(1, N_Y)]

    right, left = [own], [own]
    xs = [to_experts(own, True)]
    for k in range(1, 4):
        near = along_z(right[-1][0], 1), along_z(left[-1][0], -1)
        away = along_z(right[-1][1], 1), along_z(left[-1][1], -1)
        right.append((near[0], away[0]))
        left.append((near[1], away[1]))
        xs.append(to_experts([*left[k], *right[k]], False))
    ends = [along_z(right[3][0], 1), along_z(left[3][1], -1)]
    xs.append(to_experts(ends, True))

    ys = [None] * 5
    for n in range(5):
        ys[n] = expert(xs[n], *weights)
    rets = [to_tokens(ys[n]) for n in range(5)]

    half = jax.ShapeDtypeStruct((TOK, HALF), BF)
    wide = jax.ShapeDtypeStruct((TOK, HALF), F32)
    d0, u1 = sums(far_kernel, at, ends[:1], rets[4], (), [half] * 2)
    for k in (3, 2, 1):
        shapes = [half, wide, wide, half] if k == 3 else [wide] * 4
        pu0, pu1, pd0, pd1 = sums(two_kernel, at, [left[k][0], right[k][0]], rets[k], (), shapes)
        if k == 3:
            u0, d1 = pu0, pd1
        else:
            u0, d1 = along_z(u0, 1), along_z(d1, -1)
            u0, d1 = join(pu0, pd1, u0, d1)
        u1, d0 = along_z(u1, 1), along_z(d0, -1)
        u1, d0 = join(pu1, pd0, u1, d0)
    alone = [jax.ShapeDtypeStruct((TOK, D), F32)]
    (total,) = sums(own_kernel, at, own[:1], rets[0], (hidden,), alone)
    u0, d1 = along_z(u0, 1), along_z(d1, -1)
    u1, d0 = along_z(u1, 1), along_z(d0, -1)
    return finish(total, u0, u1, d0, d1)


def solution(mesh):
    return jax.shard_map(
        body,
        mesh=mesh,
        in_specs=(
            P("expert", "dp", None),
            P("expert", "dp", None),
            P("expert", "dp", None),
            P("expert", "dp", None),
            P("expert", "dp", None),
            P("dp", None),
            P(("dp", "expert"), None),
            P(),
            P("expert", None, None),
            P("expert", None, None),
            P("expert", None, None),
            P("dp", "expert", None, None),
            P("dp", "expert", None, None),
        ),
        out_specs=P("expert", "dp", None),
        check_vma=False,
    )
```

```python
import functools

import jax
import jax.numpy as jnp
from jax import lax
from jax.experimental import pallas as pl
from jax.experimental.pallas import tpu as pltpu
from jax.sharding import PartitionSpec as P


HEADS = 16
NOPE = 128
ROPE = 64
V_DIM = 128
TOP = 6
EPSILON = 1e-06


N_DP = 8
N_X = 4
N_Y = 4
N_Z = 8
N_EXPERT = N_Y * N_Z
STREAMS = 2
T_DEV = 64
TOK = STREAMS * T_DEV
SLOTS = 36
PAIR = 2 * SLOTS
D = 2048
FF = 704
LENGTH = 2048
HALF = D // 2
META = 8
BLOCK = TOK + META
VMEM = pltpu.MemorySpace.VMEM
BF = jnp.bfloat16
F32 = jnp.float32


def params(mib=40):
    return pltpu.CompilerParams(vmem_limit_bytes=mib << 20)


def whole(n):
    return [pl.BlockSpec(memory_space=VMEM) for _ in range(n)]


GROUP = 8


def pack_kernel(s, q_ref, k_ref, r_ref, v_ref, *rest):
    out_ref = rest[-1]
    rope = r_ref[:, s, :]
    for h in range(GROUP):
        at = h * (NOPE + ROPE)
        out_ref[0, h, 0:64, :] = q_ref[:, s, at : at + NOPE]
        out_ref[0, h, 64:128, :] = k_ref[:, s, h * NOPE : (h + 1) * NOPE]
        out_ref[0, h, 128:192, :] = v_ref[:, s, h * V_DIM : (h + 1) * V_DIM]
        out_ref[0, h, 192:256, :] = jnp.concatenate(
            [q_ref[:, s, at + NOPE : at + NOPE + ROPE], rope], axis=1
        )


def pack(s, first, steps, q, k, r, v, *part):
    wide = GROUP * (NOPE + ROPE)
    return pl.pallas_call(
        functools.partial(pack_kernel, s),
        grid=(steps,),
        out_shape=jax.ShapeDtypeStruct((STREAMS, HEADS, 256, 128), BF),
        in_specs=[
            pl.BlockSpec((T_DEV, STREAMS, wide), lambda i: (0, 0, first + i)),
            pl.BlockSpec((T_DEV, STREAMS, GROUP * NOPE), lambda i: (0, 0, first + i)),
            pl.BlockSpec((T_DEV, STREAMS, ROPE), lambda i: (0, 0, 0)),
            pl.BlockSpec((T_DEV, STREAMS, GROUP * V_DIM), lambda i: (0, 0, first + i)),
        ]
        + [pl.BlockSpec(memory_space=pl.ANY)] * len(part),
        out_specs=pl.BlockSpec((1, GROUP, 256, 128), lambda i: (s, first + i, 0, 0)),
        input_output_aliases={4: 0} if part else {},
        compiler_params=params(16),
        name="pack",
    )(q, k, r, v, *part)


QB = 256


def attend_kernel(split_ref, x_ref, o_ref, k_scr, v_scr):
    scale = (NOPE + ROPE) ** -0.5
    split = split_ref[0]
    log2e = 1.4426950408889634
    zero = jnp.zeros((T_DEV, ROPE), BF)
    for e in range(N_EXPERT):
        rows = slice(e * T_DEV, (e + 1) * T_DEV)
        k_scr[rows, 0:NOPE] = x_ref[e, 64:128, :]
        k_scr[rows, NOPE:256] = jnp.concatenate([x_ref[e, 192:256, 64:128], zero], axis=1)
        v_scr[rows, :] = x_ref[e, 128:192, :]
    per = QB // T_DEV
    for b in range(LENGTH // QB):
        n = (b + 1) * QB
        q = jnp.concatenate(
            [
                jnp.concatenate([x_ref[b * per + j, 0:64, :] for j in range(per)], axis=0),
                jnp.concatenate([x_ref[b * per + j, 192:256, :] for j in range(per)], axis=0),
            ],
            axis=1,
        )
        lane = lax.broadcasted_iota(jnp.int32, (QB, 256), 1)
        q = jnp.where(lane < NOPE + ROPE, q, jnp.zeros_like(q))
        scores = lax.dot_general(
            q, k_scr[0:n, :], (((1,), (1,)), ((), ())), preferred_element_type=F32
        )
        row = b * QB + lax.broadcasted_iota(jnp.int32, (QB, 1), 0)
        col = lax.broadcasted_iota(jnp.int32, (QB, n), 1)
        low = jnp.where(row >= split, split, 0)
        scores = jnp.where((col <= row) & (col >= low), scores, -1e30)
        peak = jnp.max(scores, axis=1, keepdims=True)
        raised = jnp.exp2((scores - peak) * (scale * log2e))
        total = jnp.sum(raised, axis=1, keepdims=True)
        mixed = jnp.dot(raised.astype(BF), v_scr[0:n, :], preferred_element_type=F32)
        mixed = (mixed / total).astype(BF)
        for j in range(per):
            o_ref[b * per + j] = mixed[j * T_DEV : (j + 1) * T_DEV, :]


def attend(split, x):
    return pl.pallas_call(
        attend_kernel,
        out_shape=jax.ShapeDtypeStruct((32, T_DEV, V_DIM), BF),
        in_specs=[pl.BlockSpec(memory_space=pltpu.MemorySpace.SMEM)] + whole(1),
        out_specs=pl.BlockSpec(memory_space=VMEM),
        scratch_shapes=[pltpu.VMEM((LENGTH, 256), BF), pltpu.VMEM((LENGTH, V_DIM), BF)],
        compiler_params=params(),
        name="attend",
    )(split, x)


PIECE = D // N_DP


def place_kernel(at_ref, x0, x1, x2, x3, top_ref, bottom_ref, scr):
    rows = PIECE // N_Y
    for k, x in enumerate((x0, x1, x2, x3)):
        start = pl.multiple_of(lax.rem(at_ref[0] + (N_Y - k), N_Y) * rows, rows)
        scr[pl.ds(start, rows), :] = x[...]
    top_ref[...] = scr[: PIECE // 2, :]
    bottom_ref[...] = scr[PIECE // 2 :, :]


def place(at, pieces):
    return pl.pallas_call(
        place_kernel,
        out_shape=[jax.ShapeDtypeStruct((PIECE // 2, D), BF)] * 2,
        in_specs=[pl.BlockSpec(memory_space=pltpu.MemorySpace.SMEM)] + whole(N_Y),
        out_specs=whole(2),
        scratch_shapes=[pltpu.VMEM((PIECE, D), BF)],
        compiler_params=params(16),
        name="place",
    )(at, *pieces)


def unfold_kernel(at_ref, in_ref, out_ref):
    rows = in_ref.shape[0] // N_Z
    for k in range(N_Z):
        apart = (k & 1) * 4 + (k & 2) + (k >> 2)
        start = pl.multiple_of((at_ref[0] ^ apart) * rows, rows)
        out_ref[pl.ds(start, rows), :] = in_ref[k * rows : (k + 1) * rows, :]


def unfold(at, x):
    return pl.pallas_call(
        unfold_kernel,
        out_shape=jax.ShapeDtypeStruct(x.shape, BF),
        in_specs=[pl.BlockSpec(memory_space=pltpu.MemorySpace.SMEM)] + whole(1),
        out_specs=pl.BlockSpec(memory_space=VMEM),
        compiler_params=params(16),
        name="unfold",
    )(at, x)


def project_kernel(which_ref, x_ref, *refs):
    w_refs = refs[: 2 * N_DP]
    res_ref, gain_ref, meta_ref, hid_ref, near_ref, away_ref = refs[2 * N_DP :]
    pieces = []
    for k in range(N_DP):
        first = which_ref[k]
        pieces.append(
            jnp.concatenate(
                [
                    jnp.concatenate([x_ref[s, first + j] for j in range(PIECE // V_DIM)], axis=1)
                    for s in range(STREAMS)
                ],
                axis=0,
            )
        )
    square = jnp.zeros((TOK, 1), F32)
    for n in range(0, D, 256):
        cols = slice(n, n + 256)
        acc = jnp.concatenate([res_ref[:, s, cols] for s in range(STREAMS)], axis=0).astype(F32)
        for k, a in enumerate(pieces):
            w = jnp.concatenate([w_refs[2 * k][:, cols], w_refs[2 * k + 1][:, cols]], axis=0)
            acc = acc + jnp.dot(a, w, preferred_element_type=F32)
        hid_ref[:, cols] = acc
        square = square + jnp.sum(acc * acc, axis=1, keepdims=True)
    scale = lax.rsqrt(square / D + EPSILON)
    for n, out_ref in ((0, near_ref), (HALF, away_ref)):
        cols = slice(n, n + HALF)
        normed = hid_ref[:, cols] * scale * gain_ref[:, cols].astype(F32)
        out_ref[0:TOK, :] = normed.astype(BF)
    near_ref[TOK:BLOCK, :] = meta_ref[...]


def project(which, x, ws, res, gain, meta):
    return pl.pallas_call(
        project_kernel,
        out_shape=(
            jax.ShapeDtypeStruct((TOK, D), F32),
            jax.ShapeDtypeStruct((BLOCK, HALF), BF),
            jax.ShapeDtypeStruct((TOK, HALF), BF),
        ),
        in_specs=[pl.BlockSpec(memory_space=pltpu.MemorySpace.SMEM)] + whole(4 + len(ws)),
        out_specs=whole(3),
        compiler_params=params(),
        name="project",
    )(which, x.reshape(STREAMS, HEADS, T_DEV, V_DIM), *ws, res, gain, meta)


ALONE = 40


def one_hot(meta, expert, slots):
    named = meta[:, 0:TOK].astype(F32)
    rows = lax.broadcasted_iota(jnp.int32, named.shape, 0)
    match = jnp.where((named == expert) & (rows < TOP), 1.0, 0.0)
    member = jnp.sum(match, axis=0, keepdims=True)
    token = lax.broadcasted_iota(jnp.int32, (TOK, TOK), 0)
    other = lax.broadcasted_iota(jnp.int32, (TOK, TOK), 1)
    before = jnp.where(token < other, 1.0, 0.0).astype(BF)
    rank = jnp.dot(
        jnp.broadcast_to(member, (8, TOK)).astype(BF), before, preferred_element_type=F32
    )[0:1, :]
    slot = lax.broadcasted_iota(jnp.int32, (slots, TOK), 0).astype(F32)
    return jnp.where((slot == rank) & (member > 0.5), 1.0, 0.0), match


def expert_at(at_ref, k):
    return (lax.rem(at_ref[0] + k, N_Y) * N_Z + at_ref[1]).astype(F32)


def select_two_kernel(at_ref, a_ref, a_rest, b_ref, b_rest, *outs):
    none = jnp.zeros((SLOTS, TOK), F32)
    picks = []
    for k in range(N_Y):
        hot_a, _ = one_hot(a_ref[TOK:BLOCK, :], expert_at(at_ref, k), SLOTS)
        hot_b, _ = one_hot(b_ref[TOK:BLOCK, :], expert_at(at_ref, k), SLOTS)
        picks += [jnp.concatenate([hot_a, none], axis=1), jnp.concatenate([none, hot_b], axis=1)]
    picks = jnp.concatenate(picks, axis=0).astype(BF)
    for n, a, b in ((0, a_ref, b_ref), (HALF, a_rest, b_rest)):
        rows = jnp.concatenate([a[0:TOK, :], b[0:TOK, :]], axis=0)
        chosen = jnp.dot(picks, rows, preferred_element_type=F32).astype(BF)
        for k in range(N_Y):
            outs[k][:, n : n + HALF] = chosen[k * PAIR : (k + 1) * PAIR, :]


def select_one_kernel(at_ref, *refs):
    parts, outs = refs[:-N_Y], refs[-N_Y:]
    meta = parts[0][TOK:BLOCK, :]
    picks = [one_hot(meta, expert_at(at_ref, k), ALONE)[0] for k in range(N_Y)]
    picks = jnp.concatenate(picks, axis=0).astype(BF)
    start = 0
    for part in parts:
        wide = part.shape[1]
        chosen = jnp.dot(picks, part[0:TOK, :], preferred_element_type=F32).astype(BF)
        for k in range(N_Y):
            outs[k][:, start : start + wide] = chosen[k * ALONE : (k + 1) * ALONE, :]
        start += wide


def select(at, parts, alone):
    return pl.pallas_call(
        select_one_kernel if alone else select_two_kernel,
        out_shape=[jax.ShapeDtypeStruct((ALONE if alone else PAIR, D), BF)] * N_Y,
        in_specs=[pl.BlockSpec(memory_space=pltpu.MemorySpace.SMEM)] + whole(len(parts)),
        out_specs=whole(N_Y),
        compiler_params=params(),
        name="select",
    )(at, *parts)


EK = 512


def expert_kernel(n, *refs):
    xs, (gate_ref, up_ref, down_ref) = refs[:n], refs[n : n + 3]
    ys, (g_scr, u_scr) = refs[n + 3 : 2 * n + 3], refs[2 * n + 3 :]
    step = pl.program_id(0)
    rows = jnp.concatenate([x[...] for x in xs], axis=0)
    across = (((1,), (1,)), ((), ()))
    g = lax.dot_general(rows, gate_ref[0], across, preferred_element_type=F32)
    u = lax.dot_general(rows, up_ref[0], across, preferred_element_type=F32)

    @pl.when(step == 0)
    def _():
        g_scr[...] = g
        u_scr[...] = u

    @pl.when(step > 0)
    def _():
        g_scr[...] += g
        u_scr[...] += u

    @pl.when(step == pl.num_programs(0) - 1)
    def _():
        gate = g_scr[...]
        act = (gate / (1.0 + jnp.exp(-gate)) * u_scr[...]).astype(BF)
        out = jnp.dot(act, down_ref[0], preferred_element_type=F32).astype(BF)
        start = 0
        for y in ys:
            y[...] = out[start : start + y.shape[0], :]
            start += y.shape[0]


def expert(xs, gate, up, down):
    n = len(xs)
    total = sum(x.shape[0] for x in xs)
    return pl.pallas_call(
        functools.partial(expert_kernel, n),
        grid=(D // EK,),
        out_shape=[jax.ShapeDtypeStruct(x.shape, BF) for x in xs],
        in_specs=[pl.BlockSpec((x.shape[0], EK), lambda i: (0, i)) for x in xs]
        + [
            pl.BlockSpec((1, FF, EK), lambda i: (0, 0, i)),
            pl.BlockSpec((1, FF, EK), lambda i: (0, 0, i)),
            pl.BlockSpec((1, FF, D), lambda i: (0, 0, 0)),
        ],
        out_specs=[pl.BlockSpec(x.shape, lambda i: (0, 0)) for x in xs],
        scratch_shapes=[pltpu.VMEM((total, FF), F32), pltpu.VMEM((total, FF), F32)],
        compiler_params=params(),
        name="expert",
    )(*xs, gate, up, down)


def weighted(at_ref, meta, slots, first, height, rows):
    high = meta[:, TOK : 2 * TOK].astype(F32)
    low = meta[:, 2 * TOK : 3 * TOK].astype(F32)
    highs, lows = [], []
    before, after = first, height - first - slots
    for k in range(N_Y):
        hot, match = one_hot(meta, expert_at(at_ref, k), slots)
        for scale, into in ((high, highs), (low, lows)):
            if before:
                into.append(jnp.zeros((before, TOK), F32))
            into.append(hot * jnp.sum(match * scale, axis=0, keepdims=True))
            if after:
                into.append(jnp.zeros((after, TOK), F32))
    contract = (((0,), (0,)), ((), ()))
    return sum(
        lax.dot_general(
            jnp.concatenate(w, axis=0).astype(BF), rows, contract, preferred_element_type=F32
        )
        for w in (highs, lows)
    )


def far_kernel(at_ref, meta_ref, r0, r1, r2, r3, down_ref, up_ref):
    rows = jnp.concatenate([r[...] for r in (r0, r1, r2, r3)], axis=0)
    total = weighted(at_ref, meta_ref[...], ALONE, 0, ALONE, rows).astype(BF)
    down_ref[...] = total[:, :HALF]
    up_ref[...] = total[:, HALF:]


def two_kernel(at_ref, a_ref, b_ref, r0, r1, r2, r3, up_0, up_1, down_0, down_1):
    rows = jnp.concatenate([r[...] for r in (r0, r1, r2, r3)], axis=0)
    up = weighted(at_ref, a_ref[...], SLOTS, 0, PAIR, rows)
    up_0[...] = up[:, :HALF].astype(up_0.dtype)
    up_1[...] = up[:, HALF:]
    down = weighted(at_ref, b_ref[...], SLOTS, SLOTS, PAIR, rows)
    down_0[...] = down[:, :HALF]
    down_1[...] = down[:, HALF:].astype(down_1.dtype)


def own_kernel(at_ref, meta_ref, r0, r1, r2, r3, hid_ref, out_ref):
    rows = jnp.concatenate([r[...] for r in (r0, r1, r2, r3)], axis=0)
    out_ref[...] = hid_ref[...] + weighted(at_ref, meta_ref[...], ALONE, 0, ALONE, rows)


def sums(kernel, at, blocks, rets, extra, shapes):
    def flat(x):
        return pl.BlockSpec(x.shape, lambda i: (0, 0))

    metas = [pl.BlockSpec((META, b.shape[1]), lambda i: (TOK // META, 0)) for b in blocks]
    return pl.pallas_call(
        kernel,
        grid=(1,),
        out_shape=shapes,
        in_specs=[pl.BlockSpec(memory_space=pltpu.MemorySpace.SMEM)]
        + metas
        + [flat(x) for x in (*rets, *extra)],
        out_specs=[flat(x) for x in shapes],
        compiler_params=params(),
        name="sums",
    )(at, *blocks, *rets, *extra)


def join_kernel(pa_ref, pb_ref, a_ref, b_ref, out_a, out_b):
    out_a[...] = (pa_ref[...] + a_ref[...].astype(F32)).astype(BF)
    out_b[...] = (pb_ref[...] + b_ref[...].astype(F32)).astype(BF)


def join(pa, pb, a, b):
    return pl.pallas_call(
        join_kernel,
        out_shape=[jax.ShapeDtypeStruct((TOK, HALF), BF)] * 2,
        in_specs=whole(4),
        out_specs=whole(2),
        compiler_params=params(16),
        name="join",
    )(pa, pb, a, b)


def finish_kernel(own_ref, up_0, up_1, down_0, down_1, out_ref):
    for n, up, down in ((0, up_0, down_0), (HALF, up_1, down_1)):
        cols = slice(n, n + HALF)
        total = own_ref[:, cols] + up[...].astype(F32) + down[...].astype(F32)
        for s in range(STREAMS):
            out_ref[:, s, cols] = total[s * T_DEV : (s + 1) * T_DEV, :].astype(BF)


def finish(own, *halves):
    return pl.pallas_call(
        finish_kernel,
        out_shape=jax.ShapeDtypeStruct((T_DEV, STREAMS, D), BF),
        in_specs=whole(5),
        out_specs=pl.BlockSpec(memory_space=VMEM),
        compiler_params=params(16),
        name="finish",
    )(own, *halves)


def along_z(x, k):
    pairs = [(y * N_Z + z, y * N_Z + (z + k) % N_Z) for y in range(N_Y) for z in range(N_Z)]
    return lax.ppermute(x, "expert", pairs)


def along_y(x, k):
    pairs = [(y * N_Z + z, (y + k) % N_Y * N_Z + z) for y in range(N_Y) for z in range(N_Z)]
    return lax.ppermute(x, "expert", pairs)


def across_z(x, bit):
    pairs = [(y * N_Z + z, y * N_Z + (z ^ bit)) for y in range(N_Y) for z in range(N_Z)]
    return lax.ppermute(x, "expert", pairs)


def along_dp(x, hops, swap):
    pairs = [
        (p * 2 + c, (p + hops) % N_X * 2 + (c + swap) % 2) for p in range(N_X) for c in range(2)
    ]
    return lax.ppermute(x, "dp", pairs)


def meta_rows(routes, route_weights):
    ids = routes.reshape(T_DEV, STREAMS, TOP).transpose(2, 1, 0).reshape(TOP, TOK)
    scales = route_weights.reshape(T_DEV, STREAMS, TOP).transpose(2, 1, 0).reshape(TOP, TOK)
    high = lax.reduce_precision(scales, 8, 7)
    both = jnp.concatenate([ids.astype(F32), high, scales - high], axis=1)
    return jnp.pad(both, ((0, META - TOP), (0, HALF - 3 * TOK))).astype(BF)


def body(
    queries,
    key_nope,
    key_rope,
    values,
    residual,
    segments,
    out_proj,
    norm_gain,
    expert_gate,
    expert_up,
    expert_down,
    routes,
    route_weights,
):
    me = lax.axis_index("expert")
    at = jnp.stack([me // N_Z, me % N_Z]).astype(jnp.int32)
    meta = meta_rows(routes, route_weights)

    inputs = (queries, key_nope, key_rope, values)
    slab = jnp.concatenate([out_proj, across_z(out_proj, 4)], axis=0)
    sent = pack(0, 0, 2, *inputs)
    slab = jnp.concatenate([slab, across_z(slab, 2)], axis=0)
    sent = pack(1, 0, 1, *inputs, sent)
    slab = jnp.concatenate([slab, across_z(slab, 1)], axis=0)
    sent = pack(1, 1, 1, *inputs, sent)
    got = lax.all_to_all(sent.reshape(N_EXPERT, 256, 128), "expert", 0, 0, tiled=True)
    slab = unfold(at[1:2], slab)
    slabs = [slab] + [along_y(slab, k) for k in range(1, N_Y)]
    top, bottom = place(at[0:1], slabs)
    up1 = [along_dp(w, 1, 0) for w in (top, bottom)]
    down1 = [along_dp(w, -1, 0) for w in (top, bottom)]
    far = [along_dp(up1[0], 1, 0), along_dp(down1[1], -1, 0)]
    pieces = [top, bottom, *up1, *down1, *far]
    pieces += [along_dp(w, 0, 1) for w in pieces]
    dp = lax.axis_index("dp")
    x, core = dp // 2, dp % 2
    which = jnp.stack(
        [
            ((x + n) % N_X * 2 + (core + c) % 2) * (PIECE // V_DIM)
            for c in range(2)
            for n in (0, 3, 1, 2)
        ]
    ).astype(jnp.int32)

    stream = me // HEADS
    ones = jnp.sum(segments, axis=1)
    split = LENGTH - jnp.where(stream == 0, ones[0], ones[1])
    mixed = attend(split.reshape(1), got)
    back = lax.all_to_all(mixed, "expert", 0, 0, tiled=True)
    hidden, *own = project(which, back, pieces, residual, norm_gain.reshape(1, D), meta)
    weights = (jnp.swapaxes(expert_gate, 1, 2), jnp.swapaxes(expert_up, 1, 2), expert_down)

    def to_experts(parts, alone):
        rows = select(at, parts, alone)
        return [rows[0]] + [along_y(rows[k], k) for k in range(1, N_Y)]

    def to_tokens(ys):
        return [ys[0]] + [along_y(ys[k], -k) for k in range(1, N_Y)]

    right, left = [own], [own]
    xs = [to_experts(own, True)]
    for k in range(1, 4):
        near = along_z(right[-1][0], 1), along_z(left[-1][0], -1)
        away = along_z(right[-1][1], 1), along_z(left[-1][1], -1)
        right.append((near[0], away[0]))
        left.append((near[1], away[1]))
        xs.append(to_experts([*left[k], *right[k]], False))
    ends = [along_z(right[3][0], 1), along_z(left[3][1], -1)]
    xs.append(to_experts(ends, True))

    ys = [None] * 5
    for n in range(5):
        ys[n] = expert(xs[n], *weights)
    rets = [to_tokens(ys[n]) for n in range(5)]

    half = jax.ShapeDtypeStruct((TOK, HALF), BF)
    wide = jax.ShapeDtypeStruct((TOK, HALF), F32)
    d0, u1 = sums(far_kernel, at, ends[:1], rets[4], (), [half] * 2)
    for k in (3, 2, 1):
        shapes = [half, wide, wide, half] if k == 3 else [wide] * 4
        pu0, pu1, pd0, pd1 = sums(two_kernel, at, [left[k][0], right[k][0]], rets[k], (), shapes)
        if k == 3:
            u0, d1 = pu0, pd1
        else:
            u0, d1 = along_z(u0, 1), along_z(d1, -1)
            u0, d1 = join(pu0, pd1, u0, d1)
        u1, d0 = along_z(u1, 1), along_z(d0, -1)
        u1, d0 = join(pu1, pd0, u1, d0)
    alone = [jax.ShapeDtypeStruct((TOK, D), F32)]
    (total,) = sums(own_kernel, at, own[:1], rets[0], (hidden,), alone)
    u0, d1 = along_z(u0, 1), along_z(d1, -1)
    u1, d0 = along_z(u1, 1), along_z(d0, -1)
    return finish(total, u0, u1, d0, d1)


def solution(mesh):
    return jax.shard_map(
        body,
        mesh=mesh,
        in_specs=(
            P("expert", "dp", None),
            P("expert", "dp", None),
            P("expert", "dp", None),
            P("expert", "dp", None),
            P("expert", "dp", None),
            P("dp", None),
            P(("dp", "expert"), None),
            P(),
            P("expert", None, None),
            P("expert", None, None),
            P("expert", None, None),
            P("dp", "expert", None, None),
            P("dp", "expert", None, None),
        ),
        out_specs=P("expert", "dp", None),
        check_vma=False,
    )
```
